32 devices in a mesh: grp: 16 (over z, y, core), tp: 2 (over x).
Axes of the slice: x: 2, y: 2, z: 4, core: 2. Of those that a mesh axis runs over, the one named last changes fastest.
Arguments:
- tokens: bfloat16 [1024, 6144], P('grp', 'tp'), may hold values from -6 to 6
- norm_gain: float32 [6144], replicated, may hold values from 0.25 to 1.75
- router_weight: bfloat16 [6144, 8], replicated, may hold values from -0.078125 to 0.078125
- expert_ids: int32 [1024, 2], P('grp'), may hold values from 0 to 7, all different within a row; in each aligned block of 64 rows (0 to 63, 64 to 127, ...) at most 18 rows name the same one
- gate_proj: bfloat16 [6144, 65536], P(None, ('grp', 'tp')), may hold values from -0.078125 to 0.078125
- up_proj: bfloat16 [6144, 65536], P(None, ('grp', 'tp')), may hold values from -0.078125 to 0.078125
- down_proj: bfloat16 [65536, 6144], P(('grp', 'tp')), may hold values from -0.125 to 0.125
Outputs:
- mixed: bfloat16 [1024, 6144], P('grp', 'tp')
The draws below stay inside these ranges and needn't reach their ends.
Inputs may be any that keep to these rules, and one draw needn't show every extreme that they name: `expert_ids`: each row names two different experts; within the rows of one group (aligned blocks of 64 rows) no expert is named more than 18 times, and in some group one expert is named exactly 18 times.
All inputs are finite; a program needn't handle non-finite values.
Results may differ from the reference program's by a relative error of at most 0.017.
Values may be sent and summed in bfloat16 or wider, within the bound.
A program may use at most 128 MiB of HBM per device.

```python
import math
import jax
import jax.numpy as jnp
import numpy as np
from jax import lax

D = 6144
EXPERTS = 8
FF = 8192
TOK_GRP = 64
CAP = 18
TOKENS = 1024
N_GRP = 16
N_TP = 2


def with_spikes(values, own_key, source, target, blocks, factor):
    def block_of(axis_at):
        return (jnp.arange(values.shape[axis_at]) // (values.shape[axis_at] // blocks)).reshape((-1,) + (1,) * (values.ndim - 1 - axis_at))

    first = jax.random.permutation(own_key, blocks)[block_of(target)]
    far = (block_of(target) + blocks // 2) % blocks
    return jnp.where((block_of(source) == first) | (block_of(source) == far), factor * values, values)


def levels(stream_key, dims, shards, low, top_value):
    def one(axis_at, blocks):
        steps = jax.random.uniform(jax.random.fold_in(jax.random.fold_in(stream_key, 6), axis_at), (blocks,), jnp.float32, low / len(shards), top_value / len(shards))
        return jnp.repeat(jnp.exp(steps), dims[axis_at] // blocks).reshape((-1,) + (1,) * (len(dims) - axis_at - 1))

    factor_of = one(*shards[0])
    for cut in shards[1:]:
        factor_of = factor_of * one(*cut)
    return factor_of


def deal_out(own_key, own, number, rows, amount, top, limit, skew):
    order = jax.random.permutation(own_key, amount)
    crowded, ordinary = shares(amount, rows * top, limit, skew, True), shares(amount, rows * top, limit, skew, False)
    places = jnp.arange(amount)

    def named(sizes, turn):
        used = int((sizes > 0).sum())
        fixed = max(1, used // 4)
        moved = fixed + (places - fixed + turn * (used - fixed)) % max(1, amount - fixed)
        return jnp.zeros((amount,), jnp.int32).at[order[jnp.where(places < fixed, places, moved)]].set(jnp.asarray(sizes, jnp.int32))

    sizes = jnp.where(number % 4 == 0, named(crowded, number // 4), named(ordinary, number - number // 4 - 1))
    mixed = jax.random.permutation(jax.random.fold_in(own, 3), amount)
    giver, sink = mixed[0:amount // 2 * 2:2], mixed[1:amount // 2 * 2:2]
    margin = jnp.minimum(sizes[giver] - 1, limit - sizes[sink]) // 2
    margin = jnp.where((giver == order[0]) | (sink == order[0]) | (sizes[sink] == 0), 0, jnp.maximum(margin, 0))
    moved = jax.random.randint(jax.random.fold_in(own, 4), (amount // 2,), 0, 1 << 20) % (margin + 1)
    sizes = sizes.at[giver].add(-moved).at[sink].add(moved)
    labels = jnp.searchsorted(jnp.cumsum(sizes), jnp.arange(rows * top), side="right").astype(jnp.int32)
    table = labels.reshape(top, rows).T
    table = table[jax.random.permutation(jax.random.fold_in(own, 1), rows)]
    turn = jax.random.randint(jax.random.fold_in(own, 2), (rows, 1), 0, top)
    return jnp.take_along_axis(table, (jnp.arange(top)[None, :] + turn) % top, axis=1)


def shares(amount, total, most, slope, full):
    loads = [(1 << 20) // math.isqrt(standing ** slope) + 1 for standing in range(1, amount + 1)]
    largest = most if full else min(most, max(-(-total // amount), total * loads[0] // sum(loads)))
    least = 1 if total - largest >= amount - 1 else 0
    holding, surplus = [largest] + [least] * (amount - 1), total - largest - least * (amount - 1)
    while surplus > 0:
        candidates = [i for i in range(1, amount) if holding[i] < largest] or [i for i in range(1, amount) if holding[i] < most]
        whole, left = sum([loads[i] for i in candidates]), surplus
        for i in candidates:
            more = min(most - holding[i], max(1, left * loads[i] // whole), surplus)
            holding[i] = holding[i] + more
            surplus = surplus - more
    return np.array(holding)


def gaussian(key, shape, spread, bound, cuts=(), held_as=jnp.bfloat16):
    entries = jax.random.normal(key, shape, jnp.float32) * spread
    if len(cuts) > 0:
        entries = levels(key, shape, cuts, -0.22, 0.18) * entries
    return jnp.clip(entries, min=-bound, max=bound).astype(held_as)


def gaussian_with(rng, extent, width, most, split, heavy, held_as=jnp.bfloat16):
    drawn = width * jax.random.normal(rng, extent, jnp.float32)
    if split:
        drawn = drawn * levels(rng, extent, split, -0.22, 0.18)
    return jnp.clip(with_spikes(drawn, jax.random.fold_in(rng, 3), *heavy), -most, most).astype(held_as)


def setup_inputs(seed: int = 0) -> dict:
    streams_of = jax.random.split(jax.random.key(seed), 8)
    tokens = gaussian(streams_of[0], (TOKENS, D), 1.0, 6.0, ((0, 16), (1, 2)))
    norm_gain = jnp.clip(1.0 + 0.15 * jax.random.normal(streams_of[1], (D,), jnp.float32), 0.25, 1.75)
    router_weight = gaussian(streams_of[2], (D, EXPERTS), D ** -0.5, 0.078125)
    expert_ids_keys = jax.random.split(jax.random.fold_in(streams_of[3], 1), TOKENS // TOK_GRP)
    expert_ids_turns = jax.random.permutation(jax.random.fold_in(streams_of[3], 3), TOKENS // TOK_GRP)
    expert_ids = jax.vmap(lambda own, number: deal_out(jax.random.fold_in(streams_of[3], 2), own, number, TOK_GRP, EXPERTS, 2, CAP, 1))(expert_ids_keys, expert_ids_turns).reshape((TOKENS, 2))
    gate_proj = gaussian(streams_of[4], (D, EXPERTS * FF), D ** -0.5, 0.078125, ((1, 32),))
    up_proj = gaussian(streams_of[5], (D, EXPERTS * FF), D ** -0.5, 0.078125, ((1, 32),))
    down_proj = gaussian_with(streams_of[6], (EXPERTS * FF, D), FF ** -0.5, 0.125, ((0, 32),), (0, 1, 32, 2.75))
    return dict(tokens=tokens, norm_gain=norm_gain, router_weight=router_weight, expert_ids=expert_ids, gate_proj=gate_proj, up_proj=up_proj, down_proj=down_proj)


def reference(tokens, norm_gain, router_weight, expert_ids, gate_proj, up_proj, down_proj):
    epsilon = 1e-05
    values = tokens.astype(jnp.float32)
    mean_square = lax.optimization_barrier(jnp.mean(values * values, axis=-1, keepdims=True))
    normed = (values * lax.rsqrt(mean_square + epsilon) * norm_gain).astype(jnp.bfloat16)
    logits = jnp.dot(normed, router_weight, preferred_element_type=jnp.float32)
    chosen = jnp.take_along_axis(logits, expert_ids, axis=1)
    gate_first = 1.0 / (1.0 + jnp.exp(chosen[:, 1] - chosen[:, 0]))
    gate_second = 1.0 / (1.0 + jnp.exp(chosen[:, 0] - chosen[:, 1]))
    gates = jnp.stack([gate_first, gate_second], axis=1)
    owners = N_GRP // EXPERTS
    slice_width = FF // (owners * N_TP)
    group_ids = expert_ids.reshape(N_GRP, TOK_GRP, 2)
    group_gates = gates.reshape(N_GRP, TOK_GRP, 2)
    mixed = jnp.zeros((TOKENS, D), jnp.float32)
    for expert in range(EXPERTS):
        hits = (group_ids == expert).astype(jnp.int32)
        routed = lax.optimization_barrier(jnp.sum(hits, axis=-1))
        gate_table = lax.optimization_barrier(jnp.sum(group_gates * hits.astype(jnp.float32), axis=-1))
        order = jnp.argsort(1 - routed, axis=1, stable=True)[:, :CAP].astype(jnp.int32)
        valid = jnp.take_along_axis(routed, order, axis=1).astype(jnp.float32)
        token_index = (order + jnp.arange(N_GRP, dtype=jnp.int32)[:, None] * TOK_GRP).reshape(-1)
        row_weight = (jnp.take_along_axis(gate_table, order, axis=1) * valid).reshape(-1)
        row_block = normed[token_index]
        total = jnp.zeros((N_GRP * CAP, D), jnp.float32)
        for quarter in range(owners):
            quarter_sum = jnp.zeros((N_GRP * CAP, D), jnp.float32)
            for piece in range(N_TP):
                column = expert * FF + (quarter * N_TP + piece) * slice_width
                gate_act = jnp.dot(row_block, gate_proj[:, column:column + slice_width], preferred_element_type=jnp.float32)
                up_act = jnp.dot(row_block, up_proj[:, column:column + slice_width], preferred_element_type=jnp.float32)
                hidden = (jax.nn.silu(gate_act) * up_act).astype(jnp.bfloat16)
                partial_out = jnp.dot(hidden, down_proj[column:column + slice_width], preferred_element_type=jnp.float32).astype(jnp.bfloat16)
                quarter_sum = quarter_sum + lax.optimization_barrier(partial_out).astype(jnp.float32)
            total = total + lax.optimization_barrier(quarter_sum.astype(jnp.bfloat16)).astype(jnp.float32)
        mixed = mixed.at[token_index].add(total * row_weight[:, None])
    return mixed.astype(jnp.bfloat16)
```

```python
from functools import partial

import jax
import jax.numpy as jnp
from jax import lax
from jax.experimental import pallas as pl
from jax.experimental.pallas import tpu as pltpu
from jax.sharding import PartitionSpec as P

CAP = 18
MESH = pl.DeviceIdType.MESH


epsilon = 1e-05


def place(experts, owners, pieces):
    g, p = lax.axis_index("grp"), lax.axis_index("tp")
    return g, p, g // owners, lax.rem(g, owners)


def greet(experts, owners, pieces):
    g, p, c, k = place(experts, owners, pieces)
    barrier = pltpu.get_barrier_semaphore()
    peers = [(lax.rem(c + j, experts) * owners + k, p) for j in range(1, experts)]
    peers += [(c * owners + lax.rem(k + d, owners), p) for d in range(1, owners)]
    peers += [(g, lax.rem(p + t, pieces)) for t in range(1, pieces)]
    for peer in peers:
        pl.semaphore_signal(barrier, inc=1, device_id=peer, device_id_type=MESH)
    pl.semaphore_wait(barrier, len(peers))


def remote(src, dst, sems, index, peer):
    return pltpu.make_async_remote_copy(
        src_ref=src,
        dst_ref=dst,
        send_sem=sems.at[(0,) + index],
        recv_sem=sems.at[(1,) + index],
        device_id=peer,
        device_id_type=MESH,
    )


def slabs_of(experts, owners, pieces, capacity, width):
    for t in range(pieces):
        for s in range(experts):
            for o in range(owners):
                rows = pl.ds((s * owners + o) * capacity, capacity)
                yield (t, s, o), (rows, pl.ds(t * width, width))


def dispatch_kernel(
    experts, owners, pieces, src, rows_out, out, local, direct, core, cross, cross_core
):
    g, p, c, k = place(experts, owners, pieces)
    greet(experts, owners, pieces)
    keep = pltpu.make_async_copy(src.at[c], out.at[p, c, k], local)
    keep.start()
    sends = {}
    for j in range(1, experts):
        e = lax.rem(c + j, experts)
        sends[j] = remote(src.at[e], out.at[p, c, k], direct, (j,), (e * owners + k, p))
        sends[j].start()
    to_core, to_piece, to_cross = [], {}, []
    for j in range(experts):
        s = lax.rem(c + experts - j, experts)
        if j == 0:
            keep.wait()
        else:
            sends[j].wait_recv()
        slab = out.at[p, s, k]
        for t in range(1, pieces):
            copy = remote(slab, slab, cross, (t, j), (g, lax.rem(p + t, pieces)))
            copy.start()
            to_piece[t, j] = copy
        for d in range(1, owners):
            peer = (c * owners + lax.rem(k + d, owners), p)
            copy = remote(slab, slab, core, (d, j), peer)
            copy.start()
            to_core.append(copy)
    for j in range(experts):
        s = lax.rem(c + experts - j, experts)
        for t in range(1, pieces):
            to_piece[t, j].wait_recv()
            slab = out.at[lax.rem(p + pieces - t, pieces), s, k]
            for d in range(1, owners):
                peer = (c * owners + lax.rem(k + d, owners), p)
                copy = remote(slab, slab, cross_core, (t, d, j), peer)
                copy.start()
                to_cross.append(copy)
    for copy in to_core + to_cross:
        copy.wait()
    for copy in list(sends.values()) + list(to_piece.values()):
        copy.wait_send()
    for slab, block in slabs_of(experts, owners, pieces, *src.shape[1:]):
        rows_out[block] = out[slab]


def collect_kernel(
    experts, owners, pieces, rows_in, out, part, near, leaving, arrived, final, core, cross, back
):
    g, p, c, k = place(experts, owners, pieces)
    greet(experts, owners, pieces)
    order = list(range(1, experts)) + [0]
    near_copies, cross_copies, back_copies = {}, {}, {}
    for slab, block in slabs_of(experts, owners, pieces, *out.shape[1:]):
        part[slab] = rows_in[block]
    for t in list(range(1, pieces)) + [0]:
        for j in order:
            s = lax.rem(c + j, experts)
            piece = lax.rem(p + t, pieces)
            for d in range(1, owners):
                other = lax.rem(k + d, owners)
                copy = remote(
                    part.at[piece, s, other],
                    near.at[d - 1, t, j],
                    core,
                    (d, t, j),
                    (c * owners + other, p),
                )
                copy.start()
                near_copies[d, t, j] = copy

    def chip_sum(t, j):
        total = part[lax.rem(p + t, pieces), lax.rem(c + j, experts), k].astype(jnp.float32)
        for d in range(1, owners):
            near_copies[d, t, j].wait_recv()
            total = total + near[d - 1, t, j].astype(jnp.float32)
        return total

    for j in order:
        for t in range(1, pieces):
            leaving[t - 1, j] = chip_sum(t, j).astype(leaving.dtype)
            copy = remote(
                leaving.at[t - 1, j],
                arrived.at[t - 1, j],
                cross,
                (t, j),
                (g, lax.rem(p + t, pieces)),
            )
            copy.start()
            cross_copies[t, j] = copy
    for j in order:
        total = chip_sum(0, j)
        for t in range(1, pieces):
            cross_copies[t, j].wait_recv()
            total = total + arrived[t - 1, j].astype(jnp.float32)
        if j == 0:
            out[c] = total.astype(out.dtype)
        else:
            final[j] = total.astype(final.dtype)
            peer = (lax.rem(c + j, experts) * owners + k, p)
            copy = remote(final.at[j], out.at[c], back, (j,), peer)
            copy.start()
            back_copies[j] = copy
    for copy in back_copies.values():
        copy.wait()
    for copy in list(near_copies.values()) + list(cross_copies.values()):
        copy.wait_send()


def dispatch(outgoing, owners, pieces):
    experts, capacity, width = outgoing.shape
    dma = pltpu.SemaphoreType.DMA
    return pl.pallas_call(
        partial(dispatch_kernel, experts, owners, pieces),
        out_shape=jax.ShapeDtypeStruct(
            (experts * owners * capacity, pieces * width), outgoing.dtype
        ),
        in_specs=[pl.BlockSpec(memory_space=pltpu.VMEM)],
        out_specs=pl.BlockSpec(memory_space=pltpu.VMEM),
        scratch_shapes=[
            pltpu.VMEM((pieces, experts, owners, capacity, width), outgoing.dtype),
            dma,
            dma((2, experts)),
            dma((2, owners, experts)),
            dma((2, pieces, experts)),
            dma((2, pieces, owners, experts)),
        ],
        compiler_params=pltpu.CompilerParams(
            collective_id=0, has_side_effects=True, vmem_limit_bytes=60 * 2**20
        ),
    )(outgoing)


def collect(part, experts, owners, pieces):
    capacity, width = part.shape[0] // (experts * owners), part.shape[1] // pieces
    dma = pltpu.SemaphoreType.DMA
    slabs = lambda *lead: pltpu.VMEM(lead + (capacity, width), part.dtype)
    return pl.pallas_call(
        partial(collect_kernel, experts, owners, pieces),
        out_shape=jax.ShapeDtypeStruct((experts, capacity, width), part.dtype),
        in_specs=[pl.BlockSpec(memory_space=pltpu.VMEM)],
        out_specs=pl.BlockSpec(memory_space=pltpu.VMEM),
        scratch_shapes=[
            slabs(pieces, experts, owners),
            slabs(max(owners - 1, 1), pieces, experts),
            slabs(max(pieces - 1, 1), experts),
            slabs(max(pieces - 1, 1), experts),
            slabs(experts),
            dma((2, owners, pieces, experts)),
            dma((2, pieces, experts)),
            dma((2, experts)),
        ],
        compiler_params=pltpu.CompilerParams(
            collective_id=1, has_side_effects=True, vmem_limit_bytes=60 * 2**20
        ),
    )(part)


TILE = 16


def shifted(value, amount):
    return value >> amount


def bits_of(number):
    return number.bit_length() - 1


def unpacking(blocks, extra):
    segments = TILE // extra
    size = blocks * TILE
    row = lax.broadcasted_iota(jnp.int32, (size, size), 0)
    col = lax.broadcasted_iota(jnp.int32, (size, size), 1)
    per = blocks * extra
    row_segment, row_rest = shifted(row, bits_of(per)), row & (per - 1)
    col_block, col_rest = shifted(col, bits_of(TILE)), col & (TILE - 1)
    same = (row_segment == shifted(col_rest, bits_of(extra))) & (
        shifted(row_rest, bits_of(extra)) == col_block
    )
    same = same & ((row & (extra - 1)) == (col & (extra - 1)))
    return row, col, same


def one_hot(mask):
    return jnp.where(mask, 1.0, 0.0).astype(jnp.bfloat16)


def mm(a, b):
    return jnp.dot(a, b, preferred_element_type=jnp.float32)


def fused_kernel(
    experts, capacity, chunks, slots,
    tokens_in, gain_in, router_in, ids, gate_w, up_w, down_w, out,
    tokens, gain, router, normed, stats, scores, sel_out, mix, unpack_all, unpack_own, pack_all,
    outgoing, rows, lhs, gate_acc, up_acc, hidden, ring, rest, part, near, leaving, arrived, final, back,
    load_s, ring_s, small_s, z_s, x_s, core_s, near_s, leave_s, back_s,
):
    g, p = lax.axis_index("grp"), lax.axis_index("tp")
    c, k = g // 2, lax.rem(g, 2)
    across, twin = (g, 1 - p), (c * 2 + 1 - k, p)
    tok, width = tokens.shape
    cw = width // chunks
    extra = capacity - TILE
    segments = TILE // extra
    segw = cw // segments
    depth = ring.shape[1]
    total_rows = 2 * experts * capacity
    main_rows = 2 * experts * TILE
    halves = gate_w.shape[1] // ring.shape[2]
    tiles = 2
    tile = ring.shape[2] // tiles
    half_of = lambda own: p if own else 1 - p
    steps = [(own, ch) for ch in range(chunks) for own in (True, False)]
    yields = [(own, ch) for ch in range(chunks) for own in (False, True)]
    per_step = 2 * halves
    in_units = len(steps) * per_step
    units = in_units + len(yields) * halves

    def unit(i):
        if i < in_units:
            step, kind = divmod(i, per_step)
            n, which = divmod(kind, 2)
            own, ch = steps[step]
            row = pl.multiple_of(half_of(own) * width + ch * cw, cw)
            src = (gate_w, up_w)[which].at[pl.ds(row, depth), pl.ds(n * ring.shape[2], ring.shape[2])]
        else:
            q, n = divmod(i - in_units, halves)
            own, ch = yields[q]
            col = pl.multiple_of(half_of(own) * width + ch * cw, cw)
            src = down_w.at[pl.ds(n * depth, depth), pl.ds(col, cw)]
        return pltpu.make_async_copy(src, ring.at[i % slots], ring_s.at[i % slots])

    barrier = pltpu.get_barrier_semaphore()
    peers = [(lax.rem(c + j, experts) * 2 + k, p) for j in range(1, experts)] + [twin, across]
    for peer in peers:
        pl.semaphore_signal(barrier, inc=1, device_id=peer, device_id_type=MESH)
    start = pl.multiple_of(p * width, width)
    loads = [
        pltpu.make_async_copy(tokens_in, tokens, load_s.at[0]),
        pltpu.make_async_copy(gain_in.at[:, pl.ds(start, width)], gain, load_s.at[1]),
        pltpu.make_async_copy(router_in.at[pl.ds(start, width), :], router, load_s.at[2]),
    ]
    for load in loads:
        load.start()
    for i in range(slots):
        unit(i).start()

    lanes = lax.broadcasted_iota(jnp.int32, (tok, 128), 1)
    chosen_first = jnp.where(ids[:, 0:1] == lanes, 1.0, 0.0)
    chosen_second = jnp.where(ids[:, 1:2] == lanes, 1.0, 0.0)
    routed = chosen_first + chosen_second
    t_row = lax.broadcasted_iota(jnp.int32, (tok, tok), 0)
    t_col = lax.broadcasted_iota(jnp.int32, (tok, tok), 1)
    place_of = mm(one_hot(t_col <= t_row), routed.astype(jnp.bfloat16)) * routed
    wide = 2 * 128
    e_row = lax.broadcasted_iota(jnp.int32, (128, wide), 0)
    e_col = lax.broadcasted_iota(jnp.int32, (128, wide), 1)
    main_cols = experts * TILE
    over = e_col - main_cols
    owner = jnp.where(e_col < main_cols, shifted(e_col, bits_of(TILE)), shifted(over, bits_of(extra)))
    spread = one_hot((owner == e_row) & (e_col < experts * capacity))
    col = lax.broadcasted_iota(jnp.int32, (tok, wide), 1)
    wanted = jnp.where(col < main_cols, col & (TILE - 1), TILE + (col & (extra - 1))) + 1
    match = jnp.where(mm(place_of.astype(jnp.bfloat16), spread) == wanted.astype(jnp.float32), 1.0, 0.0)
    sel_out[...] = match.T[: experts * capacity].astype(jnp.bfloat16)

    _, _, same = unpacking(experts, extra)
    unpack_own[...] = one_hot(same)
    row, colm, same = unpacking(2 * experts, extra)
    unpack_all[...] = one_hot(same)
    row2 = lax.broadcasted_iota(jnp.int32, row.shape, 1)
    col2 = lax.broadcasted_iota(jnp.int32, row.shape, 0)
    per = 2 * experts * extra
    same = (shifted(row2, bits_of(per)) == shifted(col2 & (TILE - 1), bits_of(extra))) & (
        shifted(row2 & (per - 1), bits_of(extra)) == shifted(col2, bits_of(TILE))
    )
    pack_all[...] = one_hot(same & ((row2 & (extra - 1)) == (col2 & (extra - 1))))

    loads[0].wait()
    squares = jnp.zeros((tok, 128), jnp.float32)
    for i in range(width // 128):
        v = tokens[:, i * 128 : (i + 1) * 128].astype(jnp.float32)
        squares = squares + v * v
    stats[0] = squares
    pl.semaphore_wait(barrier, len(peers))
    stat_copy = remote(stats.at[0], stats.at[1], small_s, (0,), across)
    stat_copy.start()
    loads[1].wait()
    stat_copy.wait_recv()
    mean_square = jnp.sum(stats[0] + stats[1], axis=1, keepdims=True) / (2 * width)
    inverse = lax.rsqrt(mean_square + epsilon)

    def sends(ch, j):
        e = lax.rem(c + j, experts)
        return remote(outgoing.at[ch, e], rows.at[p, ch, k, c], z_s, (ch, j), (e * 2 + k, p))

    def forwards(ch, j):
        slab = rows.at[p, ch, k, lax.rem(c + experts - j, experts)]
        return remote(slab, slab, x_s, (ch, j), across)

    for ch in range(chunks):
        span = slice(ch * cw, (ch + 1) * cw)
        values = tokens[:, span].astype(jnp.float32)
        normed_now = (values * inverse * gain[:, span]).astype(jnp.bfloat16)
        normed[:, span] = normed_now
        picked = mm(sel_out[...], normed_now).astype(jnp.bfloat16)
        outgoing[ch, :, :, 0:cw] = picked[:main_cols].reshape(experts, TILE, cw)
        over_rows = picked[main_cols:]
        stacked = jnp.concatenate([over_rows[:, s * segw : (s + 1) * segw] for s in range(segments)], axis=0)
        r8 = lax.broadcasted_iota(jnp.int32, (main_cols, main_cols), 1)
        c8 = lax.broadcasted_iota(jnp.int32, (main_cols, main_cols), 0)
        per8 = experts * extra
        same8 = (shifted(r8, bits_of(per8)) == shifted(c8 & (TILE - 1), bits_of(extra))) & (
            shifted(r8 & (per8 - 1), bits_of(extra)) == shifted(c8, bits_of(TILE))
        )
        pack_own = one_hot(same8 & ((r8 & (extra - 1)) == (c8 & (extra - 1))))
        packed = mm(pack_own, stacked).astype(jnp.bfloat16)
        outgoing[ch, :, :, cw:] = packed.reshape(experts, TILE, segw)
        for j in range(1, experts):
            sends(ch, j).start()
        rows[p, ch, k, c] = outgoing[ch, c]
        forwards(ch, 0).start()

    loads[2].wait()
    scores[0] = jnp.zeros((tok, 128), jnp.float32)
    scores[0, :, 0:experts] = mm(normed[...], router[...])
    score_copy = remote(scores.at[0], scores.at[1], small_s, (1,), across)
    score_copy.start()

    def z_step(ch, j):
        sends(ch, j).wait_recv()
        forwards(ch, j).start()

    def twins(own, ch):
        block = rows.at[half_of(own), ch, k]
        return remote(block, block, core_s, (0 if own else 1, ch), twin)

    def to_twin(own, ch):
        twins(own, ch).start()

    def x_wait(ch):
        for j in range(experts):
            forwards(ch, j).wait_recv()
        to_twin(False, ch)

    def gather_rows(own, ch):
        h = half_of(own)
        twins(own, ch).wait_recv()
        lhs[0:main_rows] = rows[h, ch, :, :, :, 0:cw].reshape(main_rows, cw)
        packed = rows[h, ch, :, :, :, cw:].reshape(main_rows, segw)
        loose = mm(unpack_all[...], packed).astype(jnp.bfloat16)
        per = 2 * experts * extra
        lhs[main_rows:] = jnp.concatenate([loose[s * per : (s + 1) * per] for s in range(segments)], axis=1)

    def step(index, hooks):
        own, ch = steps[index]
        gather_rows(own, ch)
        first, last = index == 0, index == len(steps) - 1

        def body(it, carry):
            for at, hook in hooks.items():
                pl.when(it == at)(hook)
            n = it // tiles
            base = index * per_step + 2 * n
            slot_g, slot_u = lax.rem(base, slots), lax.rem(base + 1, slots)

            @pl.when(lax.rem(it, tiles) == 0)
            def _():
                src = gate_w.at[pl.ds(0, depth), pl.ds(0, ring.shape[2])]
                pltpu.make_async_copy(src, ring.at[slot_g], ring_s.at[slot_g]).wait()
                pltpu.make_async_copy(src, ring.at[slot_u], ring_s.at[slot_u]).wait()

            inner = pl.ds(pl.multiple_of(lax.rem(it, tiles) * tile, tile), tile)
            outer = pl.ds(pl.multiple_of(it * tile, tile), tile)
            x = lhs[...]
            gate = mm(x, ring[slot_g, :, inner])
            up = mm(x, ring[slot_u, :, inner])
            if not first:
                gate = gate + gate_acc[:, outer]
                up = up + up_acc[:, outer]
            if last:
                hidden[:, outer] = (gate / (1.0 + jnp.exp(-gate)) * up).astype(jnp.bfloat16)
            else:
                gate_acc[:, outer] = gate
                up_acc[:, outer] = up
            return carry

        lax.fori_loop(0, halves * tiles, body, 0)
        for i in range(slots + index * per_step, min(slots + (index + 1) * per_step, units)):
            unit(i).start()

    for j in range(1, experts):
        z_step(0, j)
    to_twin(True, 0)
    for ch in range(chunks):
        if ch + 1 < chunks:
            nxt = ch + 1
            z_step(nxt, 1)
            step(2 * ch, {i: partial(z_step, nxt, 2 + i) for i in range(4)})
            x_wait(ch)
            z_step(nxt, 6)
            z_step(nxt, 7)
            to_twin(True, nxt)
            step(2 * ch + 1, {})
        else:
            step(2 * ch, {2: partial(x_wait, ch)})
            step(2 * ch + 1, {})

    score_copy.wait_recv()
    logits = scores[0] + scores[1]
    first_logit = jnp.sum(logits * chosen_first, axis=1, keepdims=True)
    second_logit = jnp.sum(logits * chosen_second, axis=1, keepdims=True)
    gate_first = 1.0 / (1.0 + jnp.exp(second_logit - first_logit))
    gate_second = 1.0 / (1.0 + jnp.exp(first_logit - second_logit))
    table = gate_first * chosen_first + gate_second * chosen_second
    high = table.astype(jnp.bfloat16)
    low = (table - high.astype(jnp.float32)).astype(jnp.bfloat16)
    kept = experts * capacity
    mix[0:tok] = (mm(high, spread) * match)[:, :kept].astype(jnp.bfloat16)
    mix[tok:] = (mm(low, spread) * match)[:, :kept].astype(jnp.bfloat16)

    nears, leaves, backs = {}, {}, {}

    def produce(q):
        base = in_units + q * halves

        def body(it, carry):
            inner = pl.ds(pl.multiple_of(it * tile, tile), tile)
            result = None
            for n in range(halves):
                slot = (base + n) % slots
                if True:

                    @pl.when(it == 0)
                    def _():
                        unit(base + n).wait()

            for n in range(halves):
                slot = (base + n) % slots
                piece = mm(hidden[:, n * depth : (n + 1) * depth], ring[slot, :, inner])
                result = piece if result is None else result + piece
            result = result.astype(jnp.bfloat16)
            part[q, :, :, :, inner] = result[:main_rows].reshape(2, experts, TILE, tile)
            rest[:, inner] = result[main_rows:]
            return carry

        lax.fori_loop(0, tiles, body, 0)
        stacked = jnp.concatenate([rest[:, s * segw : (s + 1) * segw] for s in range(segments)], axis=0)
        packed = mm(pack_all[...], stacked).astype(jnp.bfloat16)
        part[q, :, :, :, cw:] = packed.reshape(2, experts, TILE, segw)
        nears[q] = remote(part.at[q, 1 - k], near.at[q], near_s, (q,), twin)
        nears[q].start()

    def leave(ch):
        q = 2 * ch
        nears[q].wait_recv()
        for j in list(range(1, experts)) + [0]:
            s = lax.rem(c + j, experts)
            both = part[q, k, s].astype(jnp.float32) + near[q, s].astype(jnp.float32)
            leaving[ch, j] = both.astype(jnp.bfloat16)
            leaves[ch, j] = remote(leaving.at[ch, j], arrived.at[ch, j], leave_s, (ch, j), across)
            leaves[ch, j].start()

    def give(ch, j):
        q = 2 * ch + 1
        s = lax.rem(c + j, experts)
        leaves[ch, j].wait_recv()
        both = part[q, k, s].astype(jnp.float32) + near[q, s].astype(jnp.float32)
        both = (both + arrived[ch, j].astype(jnp.float32)).astype(jnp.bfloat16)
        if j == 0:
            back[ch, c] = both
        else:
            final[ch, j] = both
            backs[ch, j] = remote(final.at[ch, j], back.at[ch, c], back_s, (ch, j), (s * 2 + k, p))
            backs[ch, j].start()

    def combine(ch):
        for j in range(1, experts):
            backs[ch, j].wait_recv()
        main = back[ch, :, :, 0:cw].reshape(main_cols, cw)
        packed = back[ch, :, :, cw:].reshape(main_cols, segw)
        loose = mm(unpack_own[...], packed).astype(jnp.bfloat16)
        per = experts * extra
        loose = jnp.concatenate([loose[s * per : (s + 1) * per] for s in range(segments)], axis=1)
        both = mm(mix[...], jnp.concatenate([main, loose], axis=0))
        out[:, ch * cw : (ch + 1) * cw] = (both[:tok] + both[tok:]).astype(out.dtype)

    produce(0)
    produce(1)
    leave(0)
    nears[1].wait_recv()
    for ch in range(1, chunks):
        produce(2 * ch)
        produce(2 * ch + 1)
        leave(ch)
        nears[2 * ch + 1].wait_recv()
        if ch == 1:
            for j in (1, 2):
                give(0, j)
    for ch in range(chunks):
        for j in list(range(1 if ch else 3, experts)) + [0]:
            give(ch, j)
        if ch:
            combine(ch - 1)
    combine(chunks - 1)
    for ch in range(chunks):
        for j in range(experts):
            if j:
                sends(ch, j).wait_send()
            forwards(ch, j).wait_send()
        twins(True, ch).wait_send()
        twins(False, ch).wait_send()
    for copies in (nears, leaves, backs):
        for copy in copies.values():
            copy.wait_send()
    stat_copy.wait_send()
    score_copy.wait_send()


def fused(tokens, norm_gain, router_weight, expert_ids, gate_proj, up_proj, down_proj, chunks):
    tok, width = tokens.shape
    experts, capacity, slots = router_weight.shape[1], CAP, 18
    cw = width // chunks
    extra = capacity - TILE
    segw = cw * extra // TILE
    sw = cw + segw
    local = gate_proj.shape[1]
    total = 2 * experts * capacity
    kept = experts * capacity
    dma = pltpu.SemaphoreType.DMA
    bf = lambda *shape: pltpu.VMEM(shape, jnp.bfloat16)
    fl = lambda *shape: pltpu.VMEM(shape, jnp.float32)
    anywhere = pl.BlockSpec(memory_space=pl.ANY)
    inside = pl.BlockSpec(memory_space=pltpu.VMEM)
    return pl.pallas_call(
        partial(fused_kernel, experts, capacity, chunks, slots),
        out_shape=jax.ShapeDtypeStruct((tok, width), jnp.bfloat16),
        in_specs=[anywhere, anywhere, anywhere, inside, anywhere, anywhere, anywhere],
        out_specs=inside,
        scratch_shapes=[
            bf(tok, width), fl(1, width), bf(width, experts), bf(tok, width),
            fl(2, tok, 128), fl(2, tok, 128), bf(kept, tok), bf(2 * tok, kept),
            bf(2 * experts * TILE, 2 * experts * TILE), bf(experts * TILE, experts * TILE),
            bf(2 * experts * TILE, 2 * experts * TILE),
            bf(chunks, experts, TILE, sw),
            bf(2, chunks, 2, experts, TILE, sw),
            bf(total, cw), fl(total, local), fl(total, local), bf(total, local),
            bf(slots, cw, cw),
            bf(2 * experts * extra, cw),
            bf(2 * chunks, 2, experts, TILE, sw),
            bf(2 * chunks, experts, TILE, sw),
            bf(chunks, experts, TILE, sw), bf(chunks, experts, TILE, sw),
            bf(chunks, experts, TILE, sw), bf(chunks, experts, TILE, sw),
            dma((3,)), dma((slots,)), dma((2, 2)),
            dma((2, chunks, experts)), dma((2, chunks, experts)), dma((2, 2, chunks)),
            dma((2, 2 * chunks)), dma((2, chunks, experts)), dma((2, chunks, experts)),
        ],
        compiler_params=pltpu.CompilerParams(
            collective_id=2, has_side_effects=True, vmem_limit_bytes=67043328
        ),
    )(tokens, norm_gain.reshape(1, -1), router_weight, expert_ids, gate_proj, up_proj, down_proj)


def fits(width, local, experts, owners, pieces):
    cw = local // 2
    extra = CAP - TILE
    return (
        owners == 2 and pieces == 2 and experts == 8 and width % cw == 0
        and 0 < extra and TILE % extra == 0 and cw % (128 * (TILE // extra)) == 0
    )


def per_device(tokens, norm_gain, router_weight, expert_ids, gate_proj, up_proj, down_proj):
    tok_rows, local_width = tokens.shape
    experts = router_weight.shape[1]
    groups, pieces = lax.axis_size("grp"), lax.axis_size("tp")
    owners = groups // experts
    capacity = CAP
    local = gate_proj.shape[1]
    if fits(local_width, local, experts, owners, pieces):
        chunks = local_width // (local // 2)
        return fused(
            tokens, norm_gain, router_weight, expert_ids, gate_proj, up_proj, down_proj, chunks
        )
    start = lax.axis_index("tp") * local_width
    gain = lax.dynamic_slice_in_dim(norm_gain, start, local_width)
    router = lax.dynamic_slice_in_dim(router_weight, start, local_width, axis=0)
    values = tokens.astype(jnp.float32)
    squares = jnp.sum(values * values, axis=-1)
    squares = jnp.sum(lax.all_gather(squares, "tp"), axis=0)
    mean_square = (squares / (local_width * pieces))[:, None]
    normed = (values * lax.rsqrt(mean_square + epsilon) * gain).astype(jnp.bfloat16)
    logits = jnp.dot(normed, router, preferred_element_type=jnp.float32)
    logits = jnp.sum(lax.all_gather(logits, "tp"), axis=0)
    expert_iota = jnp.arange(experts, dtype=jnp.int32)[None, :]
    chosen_first = (expert_ids[:, 0:1] == expert_iota).astype(jnp.int32)
    chosen_second = (expert_ids[:, 1:2] == expert_iota).astype(jnp.int32)
    first_logit = jnp.sum(logits * chosen_first.astype(jnp.float32), axis=-1)
    second = jnp.sum(logits * chosen_second.astype(jnp.float32), axis=-1)
    gate_first = 1.0 / (1.0 + jnp.exp(second - first_logit))
    gate_second = 1.0 / (1.0 + jnp.exp(first_logit - second))
    gate_table = gate_first[:, None] * chosen_first.astype(jnp.float32) + gate_second[
        :, None
    ] * chosen_second.astype(jnp.float32)
    routed = chosen_first + chosen_second
    slot_index = jnp.cumsum(routed, axis=0) - 1
    slot_iota = jnp.arange(capacity, dtype=jnp.int32)
    slot_picks = (slot_index.T[:, None, :] == slot_iota[None, :, None]) & (
        routed.T[:, None, :] == 1
    )
    selector = slot_picks.astype(jnp.bfloat16)
    outgoing = jnp.einsum(
        "ect,td->ecd", selector, normed, preferred_element_type=jnp.float32
    ).astype(jnp.bfloat16)
    row_block = dispatch(outgoing, owners, pieces)
    gate_act = jnp.dot(row_block, gate_proj, preferred_element_type=jnp.float32)
    up_act = jnp.dot(row_block, up_proj, preferred_element_type=jnp.float32)
    hidden = (jax.nn.silu(gate_act) * up_act).astype(jnp.bfloat16)
    partial_out = jnp.dot(hidden, down_proj, preferred_element_type=jnp.float32).astype(
        jnp.bfloat16
    )
    summed = collect(partial_out, experts, owners, pieces).astype(jnp.float32)
    combine = slot_picks.astype(jnp.float32) * gate_table.T[:, None, :]
    mixed = jnp.einsum("ect,ecd->td", combine, summed, precision=lax.Precision.HIGHEST)
    return mixed.astype(jnp.bfloat16)


def solution(mesh):
    in_specs = (
        P("grp", "tp"),
        P(),
        P(),
        P("grp", None),
        P(None, ("grp", "tp")),
        P(None, ("grp", "tp")),
        P(("grp", "tp"), None),
    )
    out_specs = P("grp", "tp")
    return jax.shard_map(
        per_device, mesh=mesh, in_specs=in_specs, out_specs=out_specs, check_vma=False
    )
```

```python
from functools import partial

import jax
import jax.numpy as jnp
from jax import lax
from jax.experimental import pallas as pl
from jax.experimental.pallas import tpu as pltpu
from jax.sharding import PartitionSpec as P

CAP = 18
MESH = pl.DeviceIdType.MESH


epsilon = 1e-05


def place(experts, owners, pieces):
    g, p = lax.axis_index("grp"), lax.axis_index("tp")
    return g, p, g // owners, lax.rem(g, owners)


def greet(experts, owners, pieces):
    g, p, c, k = place(experts, owners, pieces)
    barrier = pltpu.get_barrier_semaphore()
    peers = [(lax.rem(c + j, experts) * owners + k, p) for j in range(1, experts)]
    peers += [(c * owners + lax.rem(k + d, owners), p) for d in range(1, owners)]
    peers += [(g, lax.rem(p + t, pieces)) for t in range(1, pieces)]
    for peer in peers:
        pl.semaphore_signal(barrier, inc=1, device_id=peer, device_id_type=MESH)
    pl.semaphore_wait(barrier, len(peers))


def remote(src, dst, sems, index, peer):
    return pltpu.make_async_remote_copy(
        src_ref=src,
        dst_ref=dst,
        send_sem=sems.at[(0,) + index],
        recv_sem=sems.at[(1,) + index],
        device_id=peer,
        device_id_type=MESH,
    )


def slabs_of(experts, owners, pieces, capacity, width):
    for t in range(pieces):
        for s in range(experts):
            for o in range(owners):
                rows = pl.ds((s * owners + o) * capacity, capacity)
                yield (t, s, o), (rows, pl.ds(t * width, width))


def dispatch_kernel(
    experts, owners, pieces, src, rows_out, out, local, direct, core, cross, cross_core
):
    g, p, c, k = place(experts, owners, pieces)
    greet(experts, owners, pieces)
    keep = pltpu.make_async_copy(src.at[c], out.at[p, c, k], local)
    keep.start()
    sends = {}
    for j in range(1, experts):
        e = lax.rem(c + j, experts)
        sends[j] = remote(src.at[e], out.at[p, c, k], direct, (j,), (e * owners + k, p))
        sends[j].start()
    to_core, to_piece, to_cross = [], {}, []
    for j in range(experts):
        s = lax.rem(c + experts - j, experts)
        if j == 0:
            keep.wait()
        else:
            sends[j].wait_recv()
        slab = out.at[p, s, k]
        for t in range(1, pieces):
            copy = remote(slab, slab, cross, (t, j), (g, lax.rem(p + t, pieces)))
            copy.start()
            to_piece[t, j] = copy
        for d in range(1, owners):
            peer = (c * owners + lax.rem(k + d, owners), p)
            copy = remote(slab, slab, core, (d, j), peer)
            copy.start()
            to_core.append(copy)
    for j in range(experts):
        s = lax.rem(c + experts - j, experts)
        for t in range(1, pieces):
            to_piece[t, j].wait_recv()
            slab = out.at[lax.rem(p + pieces - t, pieces), s, k]
            for d in range(1, owners):
                peer = (c * owners + lax.rem(k + d, owners), p)
                copy = remote(slab, slab, cross_core, (t, d, j), peer)
                copy.start()
                to_cross.append(copy)
    for copy in to_core + to_cross:
        copy.wait()
    for copy in list(sends.values()) + list(to_piece.values()):
        copy.wait_send()
    for slab, block in slabs_of(experts, owners, pieces, *src.shape[1:]):
        rows_out[block] = out[slab]


def collect_kernel(
    experts, owners, pieces, rows_in, out, part, near, leaving, arrived, final, core, cross, back
):
    g, p, c, k = place(experts, owners, pieces)
    greet(experts, owners, pieces)
    order = list(range(1, experts)) + [0]
    near_copies, cross_copies, back_copies = {}, {}, {}
    for slab, block in slabs_of(experts, owners, pieces, *out.shape[1:]):
        part[slab] = rows_in[block]
    for t in list(range(1, pieces)) + [0]:
        for j in order:
            s = lax.rem(c + j, experts)
            piece = lax.rem(p + t, pieces)
            for d in range(1, owners):
                other = lax.rem(k + d, owners)
                copy = remote(
                    part.at[piece, s, other],
                    near.at[d - 1, t, j],
                    core,
                    (d, t, j),
                    (c * owners + other, p),
                )
                copy.start()
                near_copies[d, t, j] = copy

    def chip_sum(t, j):
        total = part[lax.rem(p + t, pieces), lax.rem(c + j, experts), k].astype(jnp.float32)
        for d in range(1, owners):
            near_copies[d, t, j].wait_recv()
            total = total + near[d - 1, t, j].astype(jnp.float32)
        return total

    for j in order:
        for t in range(1, pieces):
            leaving[t - 1, j] = chip_sum(t, j).astype(leaving.dtype)
            copy = remote(
                leaving.at[t - 1, j],
                arrived.at[t - 1, j],
                cross,
                (t, j),
                (g, lax.rem(p + t, pieces)),
            )
            copy.start()
            cross_copies[t, j] = copy
    for j in order:
        total = chip_sum(0, j)
        for t in range(1, pieces):
            cross_copies[t, j].wait_recv()
            total = total + arrived[t - 1, j].astype(jnp.float32)
        if j == 0:
            out[c] = total.astype(out.dtype)
        else:
            final[j] = total.astype(final.dtype)
            peer = (lax.rem(c + j, experts) * owners + k, p)
            copy = remote(final.at[j], out.at[c], back, (j,), peer)
            copy.start()
            back_copies[j] = copy
    for copy in back_copies.values():
        copy.wait()
    for copy in list(near_copies.values()) + list(cross_copies.values()):
        copy.wait_send()


def dispatch(outgoing, owners, pieces):
    experts, capacity, width = outgoing.shape
    dma = pltpu.SemaphoreType.DMA
    return pl.pallas_call(
        partial(dispatch_kernel, experts, owners, pieces),
        out_shape=jax.ShapeDtypeStruct(
            (experts * owners * capacity, pieces * width), outgoing.dtype
        ),
        in_specs=[pl.BlockSpec(memory_space=pltpu.VMEM)],
        out_specs=pl.BlockSpec(memory_space=pltpu.VMEM),
        scratch_shapes=[
            pltpu.VMEM((pieces, experts, owners, capacity, width), outgoing.dtype),
            dma,
            dma((2, experts)),
            dma((2, owners, experts)),
            dma((2, pieces, experts)),
            dma((2, pieces, owners, experts)),
        ],
        compiler_params=pltpu.CompilerParams(
            collective_id=0, has_side_effects=True, vmem_limit_bytes=60 * 2**20
        ),
    )(outgoing)


def collect(part, experts, owners, pieces):
    capacity, width = part.shape[0] // (experts * owners), part.shape[1] // pieces
    dma = pltpu.SemaphoreType.DMA
    slabs = lambda *lead: pltpu.VMEM(lead + (capacity, width), part.dtype)
    return pl.pallas_call(
        partial(collect_kernel, experts, owners, pieces),
        out_shape=jax.ShapeDtypeStruct((experts, capacity, width), part.dtype),
        in_specs=[pl.BlockSpec(memory_space=pltpu.VMEM)],
        out_specs=pl.BlockSpec(memory_space=pltpu.VMEM),
        scratch_shapes=[
            slabs(pieces, experts, owners),
            slabs(max(owners - 1, 1), pieces, experts),
            slabs(max(pieces - 1, 1), experts),
            slabs(max(pieces - 1, 1), experts),
            slabs(experts),
            dma((2, owners, pieces, experts)),
            dma((2, pieces, experts)),
            dma((2, experts)),
        ],
        compiler_params=pltpu.CompilerParams(
            collective_id=1, has_side_effects=True, vmem_limit_bytes=60 * 2**20
        ),
    )(part)


TILE = 16


def shifted(value, amount):
    return value >> amount


def bits_of(number):
    return number.bit_length() - 1


def unpacking(blocks, extra):
    segments = TILE // extra
    size = blocks * TILE
    row = lax.broadcasted_iota(jnp.int32, (size, size), 0)
    col = lax.broadcasted_iota(jnp.int32, (size, size), 1)
    per = blocks * extra
    row_segment, row_rest = shifted(row, bits_of(per)), row & (per - 1)
    col_block, col_rest = shifted(col, bits_of(TILE)), col & (TILE - 1)
    same = (row_segment == shifted(col_rest, bits_of(extra))) & (
        shifted(row_rest, bits_of(extra)) == col_block
    )
    same = same & ((row & (extra - 1)) == (col & (extra - 1)))
    return row, col, same


def one_hot(mask):
    return jnp.where(mask, 1.0, 0.0).astype(jnp.bfloat16)


def mm(a, b):
    return jnp.dot(a, b, preferred_element_type=jnp.float32)


def fused_kernel(
    experts, capacity, chunks, slots, early,
    tokens_in, gain_in, router_in, ids, gate_w, up_w, down_w, out,
    tokens, gain, router, normed, stats, scores, sel_out, mix, unpack_all, unpack_own, pack_all,
    outgoing, rows, lhs, gate_acc, up_acc, hidden, ring, rest, part, near, leaving, arrived, final, back, mixed,
    load_s, ring_s, small_s, z_s, x_s, core_s, near_s, leave_s, back_s, out_s,
):
    g, p = lax.axis_index("grp"), lax.axis_index("tp")
    c, k = g // 2, lax.rem(g, 2)
    across, twin = (g, 1 - p), (c * 2 + 1 - k, p)
    tok, width = tokens.shape
    cw = width // chunks
    extra = capacity - TILE
    segments = TILE // extra
    segw = cw // segments
    depth = ring.shape[1]
    total_rows = 2 * experts * capacity
    main_rows = 2 * experts * TILE
    halves = gate_w.shape[1] // ring.shape[2]
    tiles = 2
    tile = ring.shape[2] // tiles
    half_of = lambda own: p if own else 1 - p
    steps = [(own, ch) for ch in range(chunks) for own in (True, False)]
    yields = [(own, ch) for ch in range(chunks) for own in (False, True)]
    per_step = 2 * halves
    in_units = len(steps) * per_step
    units = in_units + len(yields) * halves

    def unit(i):
        if i < in_units:
            step, kind = divmod(i, per_step)
            n, which = divmod(kind, 2)
            own, ch = steps[step]
            row = pl.multiple_of(half_of(own) * width + ch * cw, cw)
            src = (gate_w, up_w)[which].at[pl.ds(row, depth), pl.ds(n * ring.shape[2], ring.shape[2])]
        else:
            q, n = divmod(i - in_units, halves)
            own, ch = yields[q]
            col = pl.multiple_of(half_of(own) * width + ch * cw, cw)
            src = down_w.at[pl.ds(n * depth, depth), pl.ds(col, cw)]
        return pltpu.make_async_copy(src, ring.at[i % slots], ring_s.at[i % slots])

    barrier = pltpu.get_barrier_semaphore()
    peers = [(lax.rem(c + j, experts) * 2 + k, p) for j in range(1, experts)] + [twin, across]
    for peer in peers:
        pl.semaphore_signal(barrier, inc=1, device_id=peer, device_id_type=MESH)
    start = pl.multiple_of(p * width, width)
    loads = [
        pltpu.make_async_copy(tokens_in, tokens, load_s.at[0]),
        pltpu.make_async_copy(gain_in.at[:, pl.ds(start, width)], gain, load_s.at[1]),
        pltpu.make_async_copy(router_in.at[:, pl.ds(start, width)], router, load_s.at[2]),
    ]
    for load in loads:
        load.start()

    named = lax.broadcasted_iota(jnp.int32, (128, tok), 0)
    chosen_first = jnp.where(ids[0:1, :] == named, 1.0, 0.0).T
    chosen_second = jnp.where(ids[1:2, :] == named, 1.0, 0.0).T
    routed = chosen_first + chosen_second
    t_row = lax.broadcasted_iota(jnp.int32, (tok, tok), 0)
    t_col = lax.broadcasted_iota(jnp.int32, (tok, tok), 1)
    place_of = mm(one_hot(t_col <= t_row), routed.astype(jnp.bfloat16)) * routed
    wide = 2 * 128
    e_row = lax.broadcasted_iota(jnp.int32, (128, wide), 0)
    e_col = lax.broadcasted_iota(jnp.int32, (128, wide), 1)
    main_cols = experts * TILE
    over = e_col - main_cols
    owner = jnp.where(e_col < main_cols, shifted(e_col, bits_of(TILE)), shifted(over, bits_of(extra)))
    spread = one_hot((owner == e_row) & (e_col < experts * capacity))
    col = lax.broadcasted_iota(jnp.int32, (tok, wide), 1)
    wanted = jnp.where(col < main_cols, col & (TILE - 1), TILE + (col & (extra - 1))) + 1
    match = jnp.where(mm(place_of.astype(jnp.bfloat16), spread) == wanted.astype(jnp.float32), 1.0, 0.0)
    sel_out[...] = match.T[: experts * capacity].astype(jnp.bfloat16)

    _, _, same = unpacking(experts, extra)
    unpack_own[...] = one_hot(same)
    row, colm, same = unpacking(2 * experts, extra)
    unpack_all[...] = one_hot(same)
    row2 = lax.broadcasted_iota(jnp.int32, row.shape, 1)
    col2 = lax.broadcasted_iota(jnp.int32, row.shape, 0)
    per = 2 * experts * extra
    same = (shifted(row2, bits_of(per)) == shifted(col2 & (TILE - 1), bits_of(extra))) & (
        shifted(row2 & (per - 1), bits_of(extra)) == shifted(col2, bits_of(TILE))
    )
    pack_all[...] = one_hot(same & ((row2 & (extra - 1)) == (col2 & (extra - 1))))

    loads[0].wait()
    for i in range(early):
        unit(i).start()
    squares = jnp.zeros((tok, 128), jnp.float32)
    for i in range(width // 128):
        v = tokens[:, i * 128 : (i + 1) * 128].astype(jnp.float32)
        squares = squares + v * v
    stats[0] = squares
    pl.semaphore_wait(barrier, len(peers))
    stat_copy = remote(stats.at[0], stats.at[1], small_s, (0,), across)
    stat_copy.start()
    loads[1].wait()
    stat_copy.wait_recv()
    mean_square = jnp.sum(stats[0] + stats[1], axis=1, keepdims=True) / (2 * width)
    inverse = lax.rsqrt(mean_square + epsilon)

    def sends(ch, j):
        e = lax.rem(c + j, experts)
        return remote(outgoing.at[ch, e], rows.at[p, ch, k, c], z_s, (ch, j), (e * 2 + k, p))

    def send_all(ch):
        for j in range(1, experts):
            sends(ch, j).start()

    def forwards(ch, j):
        slab = rows.at[p, ch, k, lax.rem(c + experts - j, experts)]
        return remote(slab, slab, x_s, (ch, j), across)

    for ch in range(chunks):
        span = slice(ch * cw, (ch + 1) * cw)
        values = tokens[:, span].astype(jnp.float32)
        normed_now = (values * inverse * gain[:, span]).astype(jnp.bfloat16)
        normed[:, span] = normed_now
        picked = mm(sel_out[...], normed_now).astype(jnp.bfloat16)
        outgoing[ch, :, :, 0:cw] = picked[:main_cols].reshape(experts, TILE, cw)
        over_rows = picked[main_cols:]
        stacked = jnp.concatenate([over_rows[:, s * segw : (s + 1) * segw] for s in range(segments)], axis=0)
        r8 = lax.broadcasted_iota(jnp.int32, (main_cols, main_cols), 1)
        c8 = lax.broadcasted_iota(jnp.int32, (main_cols, main_cols), 0)
        per8 = experts * extra
        same8 = (shifted(r8, bits_of(per8)) == shifted(c8 & (TILE - 1), bits_of(extra))) & (
            shifted(r8 & (per8 - 1), bits_of(extra)) == shifted(c8, bits_of(TILE))
        )
        pack_own = one_hot(same8 & ((r8 & (extra - 1)) == (c8 & (extra - 1))))
        packed = mm(pack_own, stacked).astype(jnp.bfloat16)
        outgoing[ch, :, :, cw:] = packed.reshape(experts, TILE, segw)
        if ch == 0:
            send_all(0)
        rows[p, ch, k, c] = outgoing[ch, c]
        forwards(ch, 0).start()
    for i in range(early, slots):
        unit(i).start()

    loads[2].wait()
    scores[0] = jnp.zeros((tok, 128), jnp.float32)
    scores[0, :, 0:experts] = lax.dot_general(
        normed[...], router[...], (((1,), (1,)), ((), ())), preferred_element_type=jnp.float32
    )
    score_copy = remote(scores.at[0], scores.at[1], small_s, (1,), across)
    score_copy.start()

    def z_step(ch, j):
        sends(ch, j).wait_recv()
        forwards(ch, j).start()

    def twins(own, ch):
        block = rows.at[half_of(own), ch, k]
        return remote(block, block, core_s, (0 if own else 1, ch), twin)

    def to_twin(own, ch):
        twins(own, ch).start()

    def x_wait(ch):
        for j in range(experts):
            forwards(ch, j).wait_recv()
        to_twin(False, ch)

    def gather_rows(own, ch):
        h = half_of(own)
        twins(own, ch).wait_recv()
        lhs[0:main_rows] = rows[h, ch, :, :, :, 0:cw].reshape(main_rows, cw)
        packed = rows[h, ch, :, :, :, cw:].reshape(main_rows, segw)
        loose = mm(unpack_all[...], packed).astype(jnp.bfloat16)
        per = 2 * experts * extra
        lhs[main_rows:] = jnp.concatenate([loose[s * per : (s + 1) * per] for s in range(segments)], axis=1)

    def step(index, hooks):
        own, ch = steps[index]
        gather_rows(own, ch)
        first, last = index == 0, index == len(steps) - 1

        for it in range(halves * tiles):
            if it in hooks:
                hooks[it]()
            n, part_of = divmod(it, tiles)
            base = index * per_step + 2 * n
            if part_of == 0:
                unit(base).wait()
                unit(base + 1).wait()
            inner = pl.ds(part_of * tile, tile)
            outer = pl.ds(it * tile, tile)
            x = lhs[...]
            gate = mm(x, ring[base % slots, :, inner])
            up = mm(x, ring[(base + 1) % slots, :, inner])
            if not first:
                gate = gate + gate_acc[:, outer]
                up = up + up_acc[:, outer]
            if last:
                hidden[:, outer] = (gate / (1.0 + jnp.exp(-gate)) * up).astype(jnp.bfloat16)
            else:
                gate_acc[:, outer] = gate
                up_acc[:, outer] = up
        for i in range(slots + index * per_step, min(slots + (index + 1) * per_step, units)):
            unit(i).start()

    def z_steps(ch, *js):
        for j in js:
            z_step(ch, j)
            if j == 2 and ch + 1 < chunks:
                send_all(ch + 1)

    z_steps(0, *range(1, experts))
    to_twin(True, 0)
    for ch in range(chunks):
        if ch + 1 < chunks:
            nxt = ch + 1
            z_steps(nxt, 1)
            step(2 * ch, {1: partial(z_steps, nxt, 2), 2: partial(z_steps, nxt, 3), 3: partial(z_steps, nxt, 4)})
            x_wait(ch)
            z_steps(nxt, 5)
            step(2 * ch + 1, {2: partial(z_steps, nxt, 6)})
            z_steps(nxt, 7)
            to_twin(True, nxt)
        else:
            step(2 * ch, {2: partial(x_wait, ch)})
            step(2 * ch + 1, {})

    score_copy.wait_recv()
    logits = scores[0] + scores[1]
    first_logit = jnp.sum(logits * chosen_first, axis=1, keepdims=True)
    second_logit = jnp.sum(logits * chosen_second, axis=1, keepdims=True)
    gate_first = 1.0 / (1.0 + jnp.exp(second_logit - first_logit))
    gate_second = 1.0 / (1.0 + jnp.exp(first_logit - second_logit))
    table = gate_first * chosen_first + gate_second * chosen_second
    high = table.astype(jnp.bfloat16)
    low = (table - high.astype(jnp.float32)).astype(jnp.bfloat16)
    kept = experts * capacity
    mix[0:tok] = (mm(high, spread) * match)[:, :kept].astype(jnp.bfloat16)
    mix[tok:] = (mm(low, spread) * match)[:, :kept].astype(jnp.bfloat16)

    nears, leaves, backs, results = {}, {}, {}, []

    def produce(q):
        base = in_units + q * halves

        for n in range(halves):
            unit(base + n).wait()
        for it in range(tiles):
            inner = pl.ds(it * tile, tile)
            result = None
            for n in range(halves):
                piece = mm(hidden[:, n * depth : (n + 1) * depth], ring[(base + n) % slots, :, inner])
                result = piece if result is None else result + piece
            result = result.astype(jnp.bfloat16)
            part[q, :, :, :, inner] = result[:main_rows].reshape(2, experts, TILE, tile)
            rest[:, inner] = result[main_rows:]
        stacked = jnp.concatenate([rest[:, s * segw : (s + 1) * segw] for s in range(segments)], axis=0)
        packed = mm(pack_all[...], stacked).astype(jnp.bfloat16)
        part[q, :, :, :, cw:] = packed.reshape(2, experts, TILE, segw)
        nears[q] = remote(part.at[q, 1 - k], near.at[q], near_s, (q,), twin)
        nears[q].start()

    def leave(ch):
        q = 2 * ch
        nears[q].wait_recv()
        for j in list(range(1, experts)) + [0]:
            s = lax.rem(c + j, experts)
            both = part[q, k, s].astype(jnp.float32) + near[q, s].astype(jnp.float32)
            leaving[ch, j] = both.astype(jnp.bfloat16)
            leaves[ch, j] = remote(leaving.at[ch, j], arrived.at[ch, j], leave_s, (ch, j), across)
            leaves[ch, j].start()

    def give(ch, j):
        q = 2 * ch + 1
        s = lax.rem(c + j, experts)
        leaves[ch, j].wait_recv()
        both = part[q, k, s].astype(jnp.float32) + near[q, s].astype(jnp.float32)
        both = (both + arrived[ch, j].astype(jnp.float32)).astype(jnp.bfloat16)
        if j == 0:
            back[ch, c] = both
        else:
            final[ch, j] = both
            backs[ch, j] = remote(final.at[ch, j], back.at[ch, c], back_s, (ch, j), (s * 2 + k, p))
            backs[ch, j].start()

    def combine(ch):
        for j in range(1, experts):
            backs[ch, j].wait_recv()
        main = back[ch, :, :, 0:cw].reshape(main_cols, cw)
        packed = back[ch, :, :, cw:].reshape(main_cols, segw)
        loose = mm(unpack_own[...], packed).astype(jnp.bfloat16)
        per = experts * extra
        loose = jnp.concatenate([loose[s * per : (s + 1) * per] for s in range(segments)], axis=1)
        both = mm(mix[...], jnp.concatenate([main, loose], axis=0))
        span = slice(ch * cw, (ch + 1) * cw)
        mixed[:, span] = (both[:tok] + both[tok:]).astype(out.dtype)
        results.append(pltpu.make_async_copy(mixed.at[:, span], out.at[:, span], out_s.at[ch]))
        results[-1].start()

    def gives(ch, *js):
        if js[0] == 1:
            nears[2 * ch + 1].wait_recv()
        for j in js:
            give(ch, j)

    produce(0)
    produce(1)
    leave(0)
    produce(2)
    gives(0, 1)
    produce(3)
    leave(1)
    gives(0, 2, 3)
    produce(4)
    gives(0, 4, 5)
    produce(5)
    leave(2)
    gives(0, 6, 7, 0)
    for ch in range(chunks):
        for j in range(experts):
            if j:
                sends(ch, j).wait_send()
            forwards(ch, j).wait_send()
        twins(True, ch).wait_send()
        twins(False, ch).wait_send()
    stat_copy.wait_send()
    score_copy.wait_send()
    for ch in range(1, chunks):
        gives(ch, *range(1, experts), 0)
        if ch < chunks - 1:
            combine(ch - 1)
    for copy in list(nears.values()) + list(leaves.values()):
        copy.wait_send()
    for ch in range(chunks - 2, chunks):
        combine(ch)
    for copy in backs.values():
        copy.wait_send()
    for copy in results:
        copy.wait()


def fused(tokens, norm_gain, router_weight, expert_ids, gate_proj, up_proj, down_proj, chunks):
    tok, width = tokens.shape
    experts, capacity, slots = router_weight.shape[1], CAP, 16
    cw = width // chunks
    extra = capacity - TILE
    segw = cw * extra // TILE
    sw = cw + segw
    local = gate_proj.shape[1]
    total = 2 * experts * capacity
    kept = experts * capacity
    dma = pltpu.SemaphoreType.DMA
    bf = lambda *shape: pltpu.VMEM(shape, jnp.bfloat16)
    fl = lambda *shape: pltpu.VMEM(shape, jnp.float32)
    anywhere = pl.BlockSpec(memory_space=pl.ANY)
    inside = pl.BlockSpec(memory_space=pltpu.VMEM)
    return pl.pallas_call(
        partial(fused_kernel, experts, capacity, chunks, slots, slots // 3),
        out_shape=jax.ShapeDtypeStruct((tok, width), jnp.bfloat16),
        in_specs=[anywhere, anywhere, anywhere, inside, anywhere, anywhere, anywhere],
        out_specs=anywhere,
        scratch_shapes=[
            bf(tok, width), fl(1, width), bf(experts, width), bf(tok, width),
            fl(2, tok, 128), fl(2, tok, 128), bf(kept, tok), bf(2 * tok, kept),
            bf(2 * experts * TILE, 2 * experts * TILE), bf(experts * TILE, experts * TILE),
            bf(2 * experts * TILE, 2 * experts * TILE),
            bf(chunks, experts, TILE, sw),
            bf(2, chunks, 2, experts, TILE, sw),
            bf(total, cw), fl(total, local), fl(total, local), bf(total, local),
            bf(slots, cw, cw),
            bf(2 * experts * extra, cw),
            bf(2 * chunks, 2, experts, TILE, sw),
            bf(2 * chunks, experts, TILE, sw),
            bf(chunks, experts, TILE, sw), bf(chunks, experts, TILE, sw),
            bf(chunks, experts, TILE, sw), bf(chunks, experts, TILE, sw), bf(tok, width),
            dma((3,)), dma((slots,)), dma((2, 2)),
            dma((2, chunks, experts)), dma((2, chunks, experts)), dma((2, 2, chunks)),
            dma((2, 2 * chunks)), dma((2, chunks, experts)), dma((2, chunks, experts)), dma((chunks,)),
        ],
        compiler_params=pltpu.CompilerParams(
            collective_id=2, has_side_effects=True, vmem_limit_bytes=67043328
        ),
    )(tokens, norm_gain.reshape(1, -1), router_weight.T, expert_ids.T, gate_proj, up_proj, down_proj)


def fits(width, local, experts, owners, pieces):
    cw = local // 2
    extra = CAP - TILE
    return (
        owners == 2 and pieces == 2 and experts == 8 and width % cw == 0
        and 0 < extra and TILE % extra == 0 and cw % (128 * (TILE // extra)) == 0
    )


def per_device(tokens, norm_gain, router_weight, expert_ids, gate_proj, up_proj, down_proj):
    tok_rows, local_width = tokens.shape
    experts = router_weight.shape[1]
    groups, pieces = lax.axis_size("grp"), lax.axis_size("tp")
    owners = groups // experts
    capacity = CAP
    local = gate_proj.shape[1]
    if fits(local_width, local, experts, owners, pieces):
        chunks = local_width // (local // 2)
        return fused(
            tokens, norm_gain, router_weight, expert_ids, gate_proj, up_proj, down_proj, chunks
        )
    start = lax.axis_index("tp") * local_width
    gain = lax.dynamic_slice_in_dim(norm_gain, start, local_width)
    router = lax.dynamic_slice_in_dim(router_weight, start, local_width, axis=0)
    values = tokens.astype(jnp.float32)
    squares = jnp.sum(values * values, axis=-1)
    squares = jnp.sum(lax.all_gather(squares, "tp"), axis=0)
    mean_square = (squares / (local_width * pieces))[:, None]
    normed = (values * lax.rsqrt(mean_square + epsilon) * gain).astype(jnp.bfloat16)
    logits = jnp.dot(normed, router, preferred_element_type=jnp.float32)
    logits = jnp.sum(lax.all_gather(logits, "tp"), axis=0)
    expert_iota = jnp.arange(experts, dtype=jnp.int32)[None, :]
    chosen_first = (expert_ids[:, 0:1] == expert_iota).astype(jnp.int32)
    chosen_second = (expert_ids[:, 1:2] == expert_iota).astype(jnp.int32)
    first_logit = jnp.sum(logits * chosen_first.astype(jnp.float32), axis=-1)
    second = jnp.sum(logits * chosen_second.astype(jnp.float32), axis=-1)
    gate_first = 1.0 / (1.0 + jnp.exp(second - first_logit))
    gate_second = 1.0 / (1.0 + jnp.exp(first_logit - second))
    gate_table = gate_first[:, None] * chosen_first.astype(jnp.float32) + gate_second[
        :, None
    ] * chosen_second.astype(jnp.float32)
    routed = chosen_first + chosen_second
    slot_index = jnp.cumsum(routed, axis=0) - 1
    slot_iota = jnp.arange(capacity, dtype=jnp.int32)
    slot_picks = (slot_index.T[:, None, :] == slot_iota[None, :, None]) & (
        routed.T[:, None, :] == 1
    )
    selector = slot_picks.astype(jnp.bfloat16)
    outgoing = jnp.einsum(
        "ect,td->ecd", selector, normed, preferred_element_type=jnp.float32
    ).astype(jnp.bfloat16)
    row_block = dispatch(outgoing, owners, pieces)
    gate_act = jnp.dot(row_block, gate_proj, preferred_element_type=jnp.float32)
    up_act = jnp.dot(row_block, up_proj, preferred_element_type=jnp.float32)
    hidden = (jax.nn.silu(gate_act) * up_act).astype(jnp.bfloat16)
    partial_out = jnp.dot(hidden, down_proj, preferred_element_type=jnp.float32).astype(
        jnp.bfloat16
    )
    summed = collect(partial_out, experts, owners, pieces).astype(jnp.float32)
    combine = slot_picks.astype(jnp.float32) * gate_table.T[:, None, :]
    mixed = jnp.einsum("ect,ecd->td", combine, summed, precision=lax.Precision.HIGHEST)
    return mixed.astype(jnp.bfloat16)


def solution(mesh):
    in_specs = (
        P("grp", "tp"),
        P(),
        P(),
        P("grp", None),
        P(None, ("grp", "tp")),
        P(None, ("grp", "tp")),
        P(("grp", "tp"), None),
    )
    out_specs = P("grp", "tp")
    return jax.shard_map(
        per_device, mesh=mesh, in_specs=in_specs, out_specs=out_specs, check_vma=False
    )
```

```python
from functools import partial

import jax
import jax.numpy as jnp
from jax import lax
from jax.experimental import pallas as pl
from jax.experimental.pallas import tpu as pltpu
from jax.sharding import PartitionSpec as P

CAP = 18
MESH = pl.DeviceIdType.MESH


epsilon = 1e-05


def place(experts, owners, pieces):
    g, p = lax.axis_index("grp"), lax.axis_index("tp")
    return g, p, g // owners, lax.rem(g, owners)


def greet(experts, owners, pieces):
    g, p, c, k = place(experts, owners, pieces)
    barrier = pltpu.get_barrier_semaphore()
    peers = [(lax.rem(c + j, experts) * owners + k, p) for j in range(1, experts)]
    peers += [(c * owners + lax.rem(k + d, owners), p) for d in range(1, owners)]
    peers += [(g, lax.rem(p + t, pieces)) for t in range(1, pieces)]
    for peer in peers:
        pl.semaphore_signal(barrier, inc=1, device_id=peer, device_id_type=MESH)
    pl.semaphore_wait(barrier, len(peers))


def remote(src, dst, sems, index, peer):
    return pltpu.make_async_remote_copy(
        src_ref=src,
        dst_ref=dst,
        send_sem=sems.at[(0,) + index],
        recv_sem=sems.at[(1,) + index],
        device_id=peer,
        device_id_type=MESH,
    )


def slabs_of(experts, owners, pieces, capacity, width):
    for t in range(pieces):
        for s in range(experts):
            for o in range(owners):
                rows = pl.ds((s * owners + o) * capacity, capacity)
                yield (t, s, o), (rows, pl.ds(t * width, width))


def dispatch_kernel(
    experts, owners, pieces, src, rows_out, out, local, direct, core, cross, cross_core
):
    g, p, c, k = place(experts, owners, pieces)
    greet(experts, owners, pieces)
    keep = pltpu.make_async_copy(src.at[c], out.at[p, c, k], local)
    keep.start()
    sends = {}
    for j in range(1, experts):
        e = lax.rem(c + j, experts)
        sends[j] = remote(src.at[e], out.at[p, c, k], direct, (j,), (e * owners + k, p))
        sends[j].start()
    to_core, to_piece, to_cross = [], {}, []
    for j in range(experts):
        s = lax.rem(c + experts - j, experts)
        if j == 0:
            keep.wait()
        else:
            sends[j].wait_recv()
        slab = out.at[p, s, k]
        for t in range(1, pieces):
            copy = remote(slab, slab, cross, (t, j), (g, lax.rem(p + t, pieces)))
            copy.start()
            to_piece[t, j] = copy
        for d in range(1, owners):
            peer = (c * owners + lax.rem(k + d, owners), p)
            copy = remote(slab, slab, core, (d, j), peer)
            copy.start()
            to_core.append(copy)
    for j in range(experts):
        s = lax.rem(c + experts - j, experts)
        for t in range(1, pieces):
            to_piece[t, j].wait_recv()
            slab = out.at[lax.rem(p + pieces - t, pieces), s, k]
            for d in range(1, owners):
                peer = (c * owners + lax.rem(k + d, owners), p)
                copy = remote(slab, slab, cross_core, (t, d, j), peer)
                copy.start()
                to_cross.append(copy)
    for copy in to_core + to_cross:
        copy.wait()
    for copy in list(sends.values()) + list(to_piece.values()):
        copy.wait_send()
    for slab, block in slabs_of(experts, owners, pieces, *src.shape[1:]):
        rows_out[block] = out[slab]


def collect_kernel(
    experts, owners, pieces, rows_in, out, part, near, leaving, arrived, final, core, cross, back
):
    g, p, c, k = place(experts, owners, pieces)
    greet(experts, owners, pieces)
    order = list(range(1, experts)) + [0]
    near_copies, cross_copies, back_copies = {}, {}, {}
    for slab, block in slabs_of(experts, owners, pieces, *out.shape[1:]):
        part[slab] = rows_in[block]
    for t in list(range(1, pieces)) + [0]:
        for j in order:
            s = lax.rem(c + j, experts)
            piece = lax.rem(p + t, pieces)
            for d in range(1, owners):
                other = lax.rem(k + d, owners)
                copy = remote(
                    part.at[piece, s, other],
                    near.at[d - 1, t, j],
                    core,
                    (d, t, j),
                    (c * owners + other, p),
                )
                copy.start()
                near_copies[d, t, j] = copy

    def chip_sum(t, j):
        total = part[lax.rem(p + t, pieces), lax.rem(c + j, experts), k].astype(jnp.float32)
        for d in range(1, owners):
            near_copies[d, t, j].wait_recv()
            total = total + near[d - 1, t, j].astype(jnp.float32)
        return total

    for j in order:
        for t in range(1, pieces):
            leaving[t - 1, j] = chip_sum(t, j).astype(leaving.dtype)
            copy = remote(
                leaving.at[t - 1, j],
                arrived.at[t - 1, j],
                cross,
                (t, j),
                (g, lax.rem(p + t, pieces)),
            )
            copy.start()
            cross_copies[t, j] = copy
    for j in order:
        total = chip_sum(0, j)
        for t in range(1, pieces):
            cross_copies[t, j].wait_recv()
            total = total + arrived[t - 1, j].astype(jnp.float32)
        if j == 0:
            out[c] = total.astype(out.dtype)
        else:
            final[j] = total.astype(final.dtype)
            peer = (lax.rem(c + j, experts) * owners + k, p)
            copy = remote(final.at[j], out.at[c], back, (j,), peer)
            copy.start()
            back_copies[j] = copy
    for copy in back_copies.values():
        copy.wait()
    for copy in list(near_copies.values()) + list(cross_copies.values()):
        copy.wait_send()


def dispatch(outgoing, owners, pieces):
    experts, capacity, width = outgoing.shape
    dma = pltpu.SemaphoreType.DMA
    return pl.pallas_call(
        partial(dispatch_kernel, experts, owners, pieces),
        out_shape=jax.ShapeDtypeStruct(
            (experts * owners * capacity, pieces * width), outgoing.dtype
        ),
        in_specs=[pl.BlockSpec(memory_space=pltpu.VMEM)],
        out_specs=pl.BlockSpec(memory_space=pltpu.VMEM),
        scratch_shapes=[
            pltpu.VMEM((pieces, experts, owners, capacity, width), outgoing.dtype),
            dma,
            dma((2, experts)),
            dma((2, owners, experts)),
            dma((2, pieces, experts)),
            dma((2, pieces, owners, experts)),
        ],
        compiler_params=pltpu.CompilerParams(
            collective_id=0, has_side_effects=True, vmem_limit_bytes=60 * 2**20
        ),
    )(outgoing)


def collect(part, experts, owners, pieces):
    capacity, width = part.shape[0] // (experts * owners), part.shape[1] // pieces
    dma = pltpu.SemaphoreType.DMA
    slabs = lambda *lead: pltpu.VMEM(lead + (capacity, width), part.dtype)
    return pl.pallas_call(
        partial(collect_kernel, experts, owners, pieces),
        out_shape=jax.ShapeDtypeStruct((experts, capacity, width), part.dtype),
        in_specs=[pl.BlockSpec(memory_space=pltpu.VMEM)],
        out_specs=pl.BlockSpec(memory_space=pltpu.VMEM),
        scratch_shapes=[
            slabs(pieces, experts, owners),
            slabs(max(owners - 1, 1), pieces, experts),
            slabs(max(pieces - 1, 1), experts),
            slabs(max(pieces - 1, 1), experts),
            slabs(experts),
            dma((2, owners, pieces, experts)),
            dma((2, pieces, experts)),
            dma((2, experts)),
        ],
        compiler_params=pltpu.CompilerParams(
            collective_id=1, has_side_effects=True, vmem_limit_bytes=60 * 2**20
        ),
    )(part)


TILE = 16


def shifted(value, amount):
    return value >> amount


def bits_of(number):
    return number.bit_length() - 1


def unpacking(blocks, extra):
    segments = TILE // extra
    size = blocks * TILE
    row = lax.broadcasted_iota(jnp.int32, (size, size), 0)
    col = lax.broadcasted_iota(jnp.int32, (size, size), 1)
    per = blocks * extra
    row_segment, row_rest = shifted(row, bits_of(per)), row & (per - 1)
    col_block, col_rest = shifted(col, bits_of(TILE)), col & (TILE - 1)
    same = (row_segment == shifted(col_rest, bits_of(extra))) & (
        shifted(row_rest, bits_of(extra)) == col_block
    )
    same = same & ((row & (extra - 1)) == (col & (extra - 1)))
    return row, col, same


def one_hot(mask):
    return jnp.where(mask, 1.0, 0.0).astype(jnp.bfloat16)


def mm(a, b):
    return jnp.dot(a, b, preferred_element_type=jnp.float32)


def fused_kernel(
    experts, capacity, chunks, slots,
    tokens_in, gain_in, router_in, ids, gate_w, up_w, down_w, out,
    tokens, gain, router, normed, stats, scores, sel_out, mix, unpack_all, unpack_own, pack_all,
    outgoing, rows, lhs, gate_acc, up_acc, hidden, ring, rest, part, near, leaving, arrived, final, back, mixed,
    load_s, ring_s, small_s, z_s, x_s, core_s, near_s, leave_s, back_s, out_s,
):
    g, p = lax.axis_index("grp"), lax.axis_index("tp")
    c, k = g // 2, lax.rem(g, 2)
    across, twin = (g, 1 - p), (c * 2 + 1 - k, p)
    tok, width = tokens.shape
    cw = width // chunks
    extra = capacity - TILE
    segments = TILE // extra
    segw = cw // segments
    depth = ring.shape[1]
    total_rows = 2 * experts * capacity
    main_rows = 2 * experts * TILE
    halves = gate_w.shape[1] // ring.shape[2]
    tiles = 2
    tile = ring.shape[2] // tiles
    half_of = lambda own: p if own else 1 - p
    steps = [(own, ch) for ch in range(chunks) for own in (True, False)]
    yields = [(own, ch) for ch in range(chunks) for own in (False, True)]
    per_step = 2 * halves
    in_units = len(steps) * per_step
    units = in_units + len(yields) * halves

    def unit(i):
        if i < in_units:
            step, kind = divmod(i, per_step)
            n, which = divmod(kind, 2)
            own, ch = steps[step]
            row = pl.multiple_of(half_of(own) * width + ch * cw, cw)
            src = (gate_w, up_w)[which].at[pl.ds(row, depth), pl.ds(n * ring.shape[2], ring.shape[2])]
        else:
            q, n = divmod(i - in_units, halves)
            own, ch = yields[q]
            col = pl.multiple_of(half_of(own) * width + ch * cw, cw)
            src = down_w.at[pl.ds(n * depth, depth), pl.ds(col, cw)]
        return pltpu.make_async_copy(src, ring.at[i % slots], ring_s.at[i % slots])

    issued, used = [0], [0]

    def pump(count):
        for _ in range(count):
            if issued[0] < min(units, used[0] + slots):
                unit(issued[0]).start()
                issued[0] += 1

    barrier = pltpu.get_barrier_semaphore()
    peers = [(lax.rem(c + j, experts) * 2 + k, p) for j in range(1, experts)] + [twin, across]
    for peer in peers:
        pl.semaphore_signal(barrier, inc=1, device_id=peer, device_id_type=MESH)
    start = pl.multiple_of(p * width, width)
    loads = [
        pltpu.make_async_copy(tokens_in, tokens, load_s.at[0]),
        pltpu.make_async_copy(gain_in.at[:, pl.ds(start, width)], gain, load_s.at[1]),
        pltpu.make_async_copy(router_in.at[:, pl.ds(start, width)], router, load_s.at[2]),
    ]
    for load in loads:
        load.start()

    named = lax.broadcasted_iota(jnp.int32, (128, tok), 0)
    chosen_first = jnp.where(ids[0:1, :] == named, 1.0, 0.0).T
    chosen_second = jnp.where(ids[1:2, :] == named, 1.0, 0.0).T
    routed = chosen_first + chosen_second
    t_row = lax.broadcasted_iota(jnp.int32, (tok, tok), 0)
    t_col = lax.broadcasted_iota(jnp.int32, (tok, tok), 1)
    place_of = mm(one_hot(t_col <= t_row), routed.astype(jnp.bfloat16)) * routed
    wide = 2 * 128
    e_row = lax.broadcasted_iota(jnp.int32, (128, wide), 0)
    e_col = lax.broadcasted_iota(jnp.int32, (128, wide), 1)
    main_cols = experts * TILE
    over = e_col - main_cols
    owner = jnp.where(e_col < main_cols, shifted(e_col, bits_of(TILE)), shifted(over, bits_of(extra)))
    spread = one_hot((owner == e_row) & (e_col < experts * capacity))
    col = lax.broadcasted_iota(jnp.int32, (tok, wide), 1)
    wanted = jnp.where(col < main_cols, col & (TILE - 1), TILE + (col & (extra - 1))) + 1
    match = jnp.where(mm(place_of.astype(jnp.bfloat16), spread) == wanted.astype(jnp.float32), 1.0, 0.0)
    sel_out[...] = match.T[: experts * capacity].astype(jnp.bfloat16)

    _, _, same = unpacking(experts, extra)
    unpack_own[...] = one_hot(same)
    row, colm, same = unpacking(2 * experts, extra)
    unpack_all[...] = one_hot(same)
    row2 = lax.broadcasted_iota(jnp.int32, row.shape, 1)
    col2 = lax.broadcasted_iota(jnp.int32, row.shape, 0)
    per = 2 * experts * extra
    same = (shifted(row2, bits_of(per)) == shifted(col2 & (TILE - 1), bits_of(extra))) & (
        shifted(row2 & (per - 1), bits_of(extra)) == shifted(col2, bits_of(TILE))
    )
    pack_all[...] = one_hot(same & ((row2 & (extra - 1)) == (col2 & (extra - 1))))

    loads[0].wait()
    squares = jnp.zeros((tok, 128), jnp.float32)
    for i in range(width // 128):
        v = tokens[:, i * 128 : (i + 1) * 128].astype(jnp.float32)
        squares = squares + v * v
    stats[0] = squares
    pl.semaphore_wait(barrier, len(peers))
    stat_copy = remote(stats.at[0], stats.at[1], small_s, (0,), across)
    stat_copy.start()
    pump(1)
    loads[1].wait()
    stat_copy.wait_recv()
    mean_square = jnp.sum(stats[0] + stats[1], axis=1, keepdims=True) / (2 * width)
    inverse = lax.rsqrt(mean_square + epsilon)

    def sends(ch, j):
        e = lax.rem(c + j, experts)
        return remote(outgoing.at[ch, e], rows.at[p, ch, k, c], z_s, (ch, j), (e * 2 + k, p))

    def send_all(ch):
        for j in range(1, experts):
            sends(ch, j).start()

    def forwards(ch, j):
        slab = rows.at[p, ch, k, lax.rem(c + experts - j, experts)]
        return remote(slab, slab, x_s, (ch, j), across)

    for ch in range(chunks):
        span = slice(ch * cw, (ch + 1) * cw)
        values = tokens[:, span].astype(jnp.float32)
        normed_now = (values * inverse * gain[:, span]).astype(jnp.bfloat16)
        normed[:, span] = normed_now
        picked = mm(sel_out[...], normed_now).astype(jnp.bfloat16)
        outgoing[ch, :, :, 0:cw] = picked[:main_cols].reshape(experts, TILE, cw)
        over_rows = picked[main_cols:]
        stacked = jnp.concatenate([over_rows[:, s * segw : (s + 1) * segw] for s in range(segments)], axis=0)
        r8 = lax.broadcasted_iota(jnp.int32, (main_cols, main_cols), 1)
        c8 = lax.broadcasted_iota(jnp.int32, (main_cols, main_cols), 0)
        per8 = experts * extra
        same8 = (shifted(r8, bits_of(per8)) == shifted(c8 & (TILE - 1), bits_of(extra))) & (
            shifted(r8 & (per8 - 1), bits_of(extra)) == shifted(c8, bits_of(TILE))
        )
        pack_own = one_hot(same8 & ((r8 & (extra - 1)) == (c8 & (extra - 1))))
        packed = mm(pack_own, stacked).astype(jnp.bfloat16)
        outgoing[ch, :, :, cw:] = packed.reshape(experts, TILE, segw)
        if ch == 0:
            send_all(0)
        rows[p, ch, k, c] = outgoing[ch, c]
        forwards(ch, 0).start()
        pump(1)

    loads[2].wait()
    scores[0] = jnp.zeros((tok, 128), jnp.float32)
    scores[0, :, 0:experts] = lax.dot_general(
        normed[...], router[...], (((1,), (1,)), ((), ())), preferred_element_type=jnp.float32
    )
    score_copy = remote(scores.at[0], scores.at[1], small_s, (1,), across)
    score_copy.start()

    def z_step(ch, j):
        sends(ch, j).wait_recv()
        forwards(ch, j).start()

    def twins(own, ch):
        block = rows.at[half_of(own), ch, k]
        return remote(block, block, core_s, (0 if own else 1, ch), twin)

    def to_twin(own, ch):
        twins(own, ch).start()

    def x_wait(ch):
        for j in range(experts):
            forwards(ch, j).wait_recv()
        to_twin(False, ch)

    def gather_rows(own, ch):
        h = half_of(own)
        twins(own, ch).wait_recv()
        lhs[0:main_rows] = rows[h, ch, :, :, :, 0:cw].reshape(main_rows, cw)
        packed = rows[h, ch, :, :, :, cw:].reshape(main_rows, segw)
        loose = mm(unpack_all[...], packed).astype(jnp.bfloat16)
        per = 2 * experts * extra
        lhs[main_rows:] = jnp.concatenate([loose[s * per : (s + 1) * per] for s in range(segments)], axis=1)

    def step(index, hooks):
        own, ch = steps[index]
        gather_rows(own, ch)
        first, last = index == 0, index == len(steps) - 1

        for it in range(halves * tiles):
            if it in hooks:
                hooks[it]()
            pump(1)
            n, part_of = divmod(it, tiles)
            base = index * per_step + 2 * n
            if part_of == 0:
                unit(base).wait()
                unit(base + 1).wait()
            inner = pl.ds(part_of * tile, tile)
            outer = pl.ds(it * tile, tile)
            x = lhs[...]
            gate = mm(x, ring[base % slots, :, inner])
            up = mm(x, ring[(base + 1) % slots, :, inner])
            if not first:
                gate = gate + gate_acc[:, outer]
                up = up + up_acc[:, outer]
            if last:
                hidden[:, outer] = (gate / (1.0 + jnp.exp(-gate)) * up).astype(jnp.bfloat16)
            else:
                gate_acc[:, outer] = gate
                up_acc[:, outer] = up
            if part_of == tiles - 1:
                used[0] += 2

    def z_steps(ch, *js):
        for j in js:
            z_step(ch, j)
            pump(1)
            if j == 2 and ch + 1 < chunks:
                send_all(ch + 1)

    z_steps(0, *range(1, experts))
    to_twin(True, 0)
    for ch in range(chunks):
        if ch + 1 < chunks:
            nxt = ch + 1
            step(
                2 * ch,
                {
                    0: partial(z_steps, nxt, 1),
                    1: partial(z_steps, nxt, 2),
                    2: lambda: (x_wait(ch), z_steps(nxt, 3)),
                    3: partial(z_steps, nxt, 4),
                },
            )
            step(
                2 * ch + 1,
                {
                    0: partial(z_steps, nxt, 5),
                    1: partial(z_steps, nxt, 6),
                    2: lambda: (z_steps(nxt, 7), to_twin(True, nxt)),
                },
            )
        else:
            step(2 * ch, {2: partial(x_wait, ch)})
            step(2 * ch + 1, {})

    score_copy.wait_recv()
    logits = scores[0] + scores[1]
    first_logit = jnp.sum(logits * chosen_first, axis=1, keepdims=True)
    second_logit = jnp.sum(logits * chosen_second, axis=1, keepdims=True)
    gate_first = 1.0 / (1.0 + jnp.exp(second_logit - first_logit))
    gate_second = 1.0 / (1.0 + jnp.exp(first_logit - second_logit))
    table = gate_first * chosen_first + gate_second * chosen_second
    high = table.astype(jnp.bfloat16)
    low = (table - high.astype(jnp.float32)).astype(jnp.bfloat16)
    kept = experts * capacity
    mix[0:tok] = (mm(high, spread) * match)[:, :kept].astype(jnp.bfloat16)
    mix[tok:] = (mm(low, spread) * match)[:, :kept].astype(jnp.bfloat16)

    nears, leaves, backs, results = {}, {}, {}, []

    def produce(q):
        base = in_units + q * halves

        for n in range(halves):
            unit(base + n).wait()
        for it in range(tiles):
            inner = pl.ds(it * tile, tile)
            result = None
            for n in range(halves):
                piece = mm(hidden[:, n * depth : (n + 1) * depth], ring[(base + n) % slots, :, inner])
                result = piece if result is None else result + piece
            result = result.astype(jnp.bfloat16)
            part[q, :, :, :, inner] = result[:main_rows].reshape(2, experts, TILE, tile)
            rest[:, inner] = result[main_rows:]
            pump(1)
        used[0] += halves
        stacked = jnp.concatenate([rest[:, s * segw : (s + 1) * segw] for s in range(segments)], axis=0)
        packed = mm(pack_all[...], stacked).astype(jnp.bfloat16)
        part[q, :, :, :, cw:] = packed.reshape(2, experts, TILE, segw)
        nears[q] = remote(part.at[q, 1 - k], near.at[q], near_s, (q,), twin)
        nears[q].start()

    def leave(ch):
        q = 2 * ch
        nears[q].wait_recv()
        for j in list(range(1, experts)) + [0]:
            s = lax.rem(c + j, experts)
            both = part[q, k, s].astype(jnp.float32) + near[q, s].astype(jnp.float32)
            leaving[ch, j] = both.astype(jnp.bfloat16)
            leaves[ch, j] = remote(leaving.at[ch, j], arrived.at[ch, j], leave_s, (ch, j), across)
            leaves[ch, j].start()

    def give(ch, j):
        q = 2 * ch + 1
        s = lax.rem(c + j, experts)
        leaves[ch, j].wait_recv()
        both = part[q, k, s].astype(jnp.float32) + near[q, s].astype(jnp.float32)
        both = (both + arrived[ch, j].astype(jnp.float32)).astype(jnp.bfloat16)
        if j == 0:
            back[ch, c] = both
        else:
            final[ch, j] = both
            backs[ch, j] = remote(final.at[ch, j], back.at[ch, c], back_s, (ch, j), (s * 2 + k, p))
            backs[ch, j].start()

    def combine(ch):
        for j in range(1, experts):
            backs[ch, j].wait_recv()
        main = back[ch, :, :, 0:cw].reshape(main_cols, cw)
        packed = back[ch, :, :, cw:].reshape(main_cols, segw)
        loose = mm(unpack_own[...], packed).astype(jnp.bfloat16)
        per = experts * extra
        loose = jnp.concatenate([loose[s * per : (s + 1) * per] for s in range(segments)], axis=1)
        both = mm(mix[...], jnp.concatenate([main, loose], axis=0))
        span = slice(ch * cw, (ch + 1) * cw)
        mixed[:, span] = (both[:tok] + both[tok:]).astype(out.dtype)
        results.append(pltpu.make_async_copy(mixed.at[:, span], out.at[:, span], out_s.at[ch]))
        results[-1].start()

    def gives(ch, *js):
        if js[0] == 1:
            nears[2 * ch + 1].wait_recv()
        for j in js:
            give(ch, j)

    produce(0)
    produce(1)
    leave(0)
    produce(2)
    gives(0, 1)
    produce(3)
    leave(1)
    gives(0, 2, 3)
    produce(4)
    gives(0, 4, 5)
    produce(5)
    leave(2)
    gives(0, 6, 7, 0)
    for ch in range(chunks):
        for j in range(experts):
            if j:
                sends(ch, j).wait_send()
            forwards(ch, j).wait_send()
        twins(True, ch).wait_send()
        twins(False, ch).wait_send()
    stat_copy.wait_send()
    score_copy.wait_send()
    for ch in range(1, chunks):
        gives(ch, *range(1, experts), 0)
        if ch < chunks - 1:
            combine(ch - 1)
    for copy in list(nears.values()) + list(leaves.values()):
        copy.wait_send()
    for ch in range(chunks - 2, chunks):
        combine(ch)
    for copy in backs.values():
        copy.wait_send()
    for copy in results:
        copy.wait()


def fused(tokens, norm_gain, router_weight, expert_ids, gate_proj, up_proj, down_proj, chunks):
    tok, width = tokens.shape
    experts, capacity, slots = router_weight.shape[1], CAP, 16
    cw = width // chunks
    extra = capacity - TILE
    segw = cw * extra // TILE
    sw = cw + segw
    local = gate_proj.shape[1]
    total = 2 * experts * capacity
    kept = experts * capacity
    dma = pltpu.SemaphoreType.DMA
    bf = lambda *shape: pltpu.VMEM(shape, jnp.bfloat16)
    fl = lambda *shape: pltpu.VMEM(shape, jnp.float32)
    anywhere = pl.BlockSpec(memory_space=pl.ANY)
    inside = pl.BlockSpec(memory_space=pltpu.VMEM)
    return pl.pallas_call(
        partial(fused_kernel, experts, capacity, chunks, slots),
        out_shape=jax.ShapeDtypeStruct((tok, width), jnp.bfloat16),
        in_specs=[anywhere, anywhere, anywhere, inside, anywhere, anywhere, anywhere],
        out_specs=anywhere,
        scratch_shapes=[
            bf(tok, width), fl(1, width), bf(experts, width), bf(tok, width),
            fl(2, tok, 128), fl(2, tok, 128), bf(kept, tok), bf(2 * tok, kept),
            bf(2 * experts * TILE, 2 * experts * TILE), bf(experts * TILE, experts * TILE),
            bf(2 * experts * TILE, 2 * experts * TILE),
            bf(chunks, experts, TILE, sw),
            bf(2, chunks, 2, experts, TILE, sw),
            bf(total, cw), fl(total, local), fl(total, local), bf(total, local),
            bf(slots, cw, cw),
            bf(2 * experts * extra, cw),
            bf(2 * chunks, 2, experts, TILE, sw),
            bf(2 * chunks, experts, TILE, sw),
            bf(chunks, experts, TILE, sw), bf(chunks, experts, TILE, sw),
            bf(chunks, experts, TILE, sw), bf(chunks, experts, TILE, sw), bf(tok, width),
            dma((3,)), dma((slots,)), dma((2, 2)),
            dma((2, chunks, experts)), dma((2, chunks, experts)), dma((2, 2, chunks)),
            dma((2, 2 * chunks)), dma((2, chunks, experts)), dma((2, chunks, experts)), dma((chunks,)),
        ],
        compiler_params=pltpu.CompilerParams(
            collective_id=2, has_side_effects=True, vmem_limit_bytes=67043328
        ),
    )(tokens, norm_gain.reshape(1, -1), router_weight.T, expert_ids.T, gate_proj, up_proj, down_proj)


def fits(width, local, experts, owners, pieces):
    cw = local // 2
    extra = CAP - TILE
    return (
        owners == 2 and pieces == 2 and experts == 8 and width % cw == 0
        and 0 < extra and TILE % extra == 0 and cw % (128 * (TILE // extra)) == 0
    )


def per_device(tokens, norm_gain, router_weight, expert_ids, gate_proj, up_proj, down_proj):
    tok_rows, local_width = tokens.shape
    experts = router_weight.shape[1]
    groups, pieces = lax.axis_size("grp"), lax.axis_size("tp")
    owners = groups // experts
    capacity = CAP
    local = gate_proj.shape[1]
    if fits(local_width, local, experts, owners, pieces):
        chunks = local_width // (local // 2)
        return fused(
            tokens, norm_gain, router_weight, expert_ids, gate_proj, up_proj, down_proj, chunks
        )
    start = lax.axis_index("tp") * local_width
    gain = lax.dynamic_slice_in_dim(norm_gain, start, local_width)
    router = lax.dynamic_slice_in_dim(router_weight, start, local_width, axis=0)
    values = tokens.astype(jnp.float32)
    squares = jnp.sum(values * values, axis=-1)
    squares = jnp.sum(lax.all_gather(squares, "tp"), axis=0)
    mean_square = (squares / (local_width * pieces))[:, None]
    normed = (values * lax.rsqrt(mean_square + epsilon) * gain).astype(jnp.bfloat16)
    logits = jnp.dot(normed, router, preferred_element_type=jnp.float32)
    logits = jnp.sum(lax.all_gather(logits, "tp"), axis=0)
    expert_iota = jnp.arange(experts, dtype=jnp.int32)[None, :]
    chosen_first = (expert_ids[:, 0:1] == expert_iota).astype(jnp.int32)
    chosen_second = (expert_ids[:, 1:2] == expert_iota).astype(jnp.int32)
    first_logit = jnp.sum(logits * chosen_first.astype(jnp.float32), axis=-1)
    second = jnp.sum(logits * chosen_second.astype(jnp.float32), axis=-1)
    gate_first = 1.0 / (1.0 + jnp.exp(second - first_logit))
    gate_second = 1.0 / (1.0 + jnp.exp(first_logit - second))
    gate_table = gate_first[:, None] * chosen_first.astype(jnp.float32) + gate_second[
        :, None
    ] * chosen_second.astype(jnp.float32)
    routed = chosen_first + chosen_second
    slot_index = jnp.cumsum(routed, axis=0) - 1
    slot_iota = jnp.arange(capacity, dtype=jnp.int32)
    slot_picks = (slot_index.T[:, None, :] == slot_iota[None, :, None]) & (
        routed.T[:, None, :] == 1
    )
    selector = slot_picks.astype(jnp.bfloat16)
    outgoing = jnp.einsum(
        "ect,td->ecd", selector, normed, preferred_element_type=jnp.float32
    ).astype(jnp.bfloat16)
    row_block = dispatch(outgoing, owners, pieces)
    gate_act = jnp.dot(row_block, gate_proj, preferred_element_type=jnp.float32)
    up_act = jnp.dot(row_block, up_proj, preferred_element_type=jnp.float32)
    hidden = (jax.nn.silu(gate_act) * up_act).astype(jnp.bfloat16)
    partial_out = jnp.dot(hidden, down_proj, preferred_element_type=jnp.float32).astype(
        jnp.bfloat16
    )
    summed = collect(partial_out, experts, owners, pieces).astype(jnp.float32)
    combine = slot_picks.astype(jnp.float32) * gate_table.T[:, None, :]
    mixed = jnp.einsum("ect,ecd->td", combine, summed, precision=lax.Precision.HIGHEST)
    return mixed.astype(jnp.bfloat16)


def solution(mesh):
    in_specs = (
        P("grp", "tp"),
        P(),
        P(),
        P("grp", None),
        P(None, ("grp", "tp")),
        P(None, ("grp", "tp")),
        P(("grp", "tp"), None),
    )
    out_specs = P("grp", "tp")
    return jax.shard_map(
        per_device, mesh=mesh, in_specs=in_specs, out_specs=out_specs, check_vma=False
    )
```
